128 devices in a mesh: section: 8 (over x, z_hi), dp: 16 (over z_lo, y, core).
Axes of the slice: x: 4, y: 4, z: 4 (z_hi: 2, z_lo: 2; z = z_hi * 2 + z_lo), core: 2. Of those that a mesh axis runs over, the one named last changes fastest.
Arguments:
- inputs: bfloat16 [8, 128, 16384], P(None, None, 'dp'), may hold values from -6 to 6
- cotangent: bfloat16 [8, 8, 128, 1024], P('section'), may hold values from -0.5 to 0.5
- norm_gain: bfloat16 [8, 16384], P('section', 'dp'), may hold values from 0.099609375 to 1.8984375
- value_weight: bfloat16 [8, 16384, 1024], P('section', 'dp'), may hold values from -0.046875 to 0.046875
- output_weight: bfloat16 [8, 1024, 16384], P('section', None, 'dp'), may hold values from -0.1875 to 0.1875
- left_old: float32 [8, 16, 1024, 1024], P('section', 'dp'), may hold values from -0.4 to 2.4, as said below
- right_old: float32 [8, 1024, 1024], P('section', 'dp'), may hold values from -0.4 to 2.4, as said below
Outputs:
- section_outputs: bfloat16 [8, 8, 128, 16384], P('section', None, None, 'dp')
- left_stats: float32 [8, 16, 1024, 1024], P('section', 'dp')
- right_stats: float32 [8, 1024, 1024], P('section', 'dp')
The draws below stay inside these ranges and needn't reach their ends.
Inputs may be any that keep to these rules, and one draw needn't show every extreme that they name: `left_old`: symmetric in its last two dimensions. `right_old`: symmetric in its last two dimensions.
All inputs are finite; a program needn't handle non-finite values.
Results may differ from the reference program's by a relative error of at most 0.015.
Values may be sent and summed in bfloat16 or wider, within the bound.
A program may use at most 128 MiB of HBM per device.

```python
import jax
import jax.numpy as jnp
from jax import lax

D = 16384
KV = 1024
BLOCK = 1024
MICRO = 8
MB = 128
SECTIONS = 8
NB = 16
N_SECTION = 8


def symmetric(key, leading, order):
    key_noise, key_diag = jax.random.split(key)
    noise_part = jnp.clip(jax.random.normal(key_noise, leading + (order, order), jnp.float32), -4.0, 4.0) * 0.05
    diagonal = jax.random.uniform(key_diag, leading + (order,), jnp.float32, 0.5, 2.0)
    return noise_part + jnp.swapaxes(noise_part, -1, -2) + diagonal[..., None] * jnp.eye(order, dtype=jnp.float32)


def draw_left_old(key, part):
    return symmetric(jax.random.fold_in(key, 11), (SECTIONS, NB), BLOCK)


def draw_right_old(key, part):
    return symmetric(jax.random.fold_in(key, 23), (SECTIONS,), KV)


def block_scale(rng, dims, pieces, low, largest):
    factor_of = 1.0
    for dim, shards_of in pieces:
        heights = jax.random.uniform(jax.random.fold_in(jax.random.fold_in(rng, 6), dim), (shards_of,), jnp.float32, low / len(pieces), largest / len(pieces))
        factor_of = factor_of * jnp.repeat(jnp.exp(heights), dims[dim] // shards_of).reshape((-1,) + (1,) * (len(dims) - 1 - dim))
    return factor_of


def normal_values(stream_key, extent, spread, reach, cuts=(), kind=jnp.bfloat16):
    array = jax.random.normal(stream_key, extent, jnp.float32) * spread
    if len(cuts) > 0:
        array = block_scale(stream_key, extent, cuts, -0.22, 0.18) * array
    return jnp.clip(array, min=-reach, max=reach).astype(kind)


def setup_inputs(seed: int = 0) -> dict:
    keys = jax.random.split(jax.random.key(seed), 8)
    return {
        "inputs": normal_values(keys[0], (MICRO, MB, D), 1.0, 6.0, ((2, 16),)),
        "cotangent": normal_values(keys[1], (SECTIONS, MICRO, MB, KV), 0.08, 0.5, ((0, 8),)),
        "norm_gain": jnp.clip(1.0 + 0.18 * jax.random.normal(keys[2], (SECTIONS, D), jnp.float32), 0.099609375, 1.8984375).astype(jnp.bfloat16),
        "value_weight": normal_values(keys[3], (SECTIONS, D, KV), D ** -0.5, 0.046875, ((0, 8), (1, 16))),
        "output_weight": normal_values(keys[4], (SECTIONS, KV, D), KV ** -0.5, 0.1875, ((0, 8), (2, 16))),
        "left_old": draw_left_old(jax.random.fold_in(keys[7], 71), 0),
        "right_old": draw_right_old(jax.random.fold_in(keys[7], 71), 0),
    }


def reference(inputs, cotangent, norm_gain, value_weight, output_weight, left_old, right_old):
    micro_count, batch_rows, model_width = inputs.shape
    hidden_in = inputs.reshape(micro_count * batch_rows, model_width)
    outputs_all = []
    lefts_all = []
    rights_all = []
    for layer_index in range(N_SECTION):
        floats = hidden_in.astype(jnp.float32)
        scaled_in = (floats * norm_gain[layer_index].astype(jnp.float32)).astype(jnp.bfloat16)
        inv_rms = lax.rsqrt(lax.optimization_barrier(jnp.mean(floats * floats, axis=1)) + 0.25)
        products = jnp.dot(scaled_in, value_weight[layer_index], preferred_element_type=jnp.float32)
        values = (inv_rms[:, None] * products).astype(jnp.bfloat16)
        hidden_in = (floats + jnp.dot(values, output_weight[layer_index], preferred_element_type=jnp.float32)).astype(jnp.bfloat16)
        cotan_rows = cotangent[layer_index].reshape(micro_count * batch_rows, KV).astype(jnp.float32)
        weighted = (inv_rms[:, None] * cotan_rows).astype(jnp.bfloat16)
        gradient = jnp.dot(scaled_in.T, weighted, preferred_element_type=jnp.float32).astype(jnp.bfloat16)
        blocks = gradient.reshape(NB, BLOCK, KV).astype(jnp.float32)
        left_new = left_old[layer_index] + jnp.einsum('bik,bjk->bij', blocks, blocks, precision=lax.Precision.HIGHEST) / BLOCK
        right_new = right_old[layer_index] + jnp.dot(gradient.T, gradient, preferred_element_type=jnp.float32) / D
        outputs_all.append(hidden_in.reshape(micro_count, batch_rows, model_width))
        lefts_all.append(left_new)
        rights_all.append(right_new)
    return (jnp.stack(outputs_all), jnp.stack(lefts_all), jnp.stack(rights_all))
```

```python
import jax
import jax.numpy as jnp
from jax import lax
from jax.experimental import pallas as pl
from jax.experimental.pallas import tpu as pltpu
from jax.sharding import PartitionSpec as P

MESH = pl.DeviceIdType.MESH
F32 = jnp.float32
BF16 = jnp.bfloat16

D = 16384
W = 1024
KV = 1024
ROWS = 1024
T = 64
NC = ROWS // T
PLANE = 8
OWN = T // PLANE
EXT = KV + 128
Y = 4


def with_pair(rows, scalar):
    high = scalar.astype(BF16).astype(F32)
    low = scalar - high
    lane = lax.broadcasted_iota(jnp.int32, (rows.shape[0], 128), 1)
    pair = jnp.where(lane < 64, high, low)
    return jnp.concatenate([rows, pair], axis=1)


def pair_of(ext):
    return ext[:, KV : KV + 1] + ext[:, KV + 64 : KV + 65]


def kernel(
    x_hbm, cot_hbm, gain_ref, wv_hbm, wo_hbm, left_old_hbm, right_old_hbm,
    out_hbm, left_hbm, right_hbm,
    wv, wo, cot, xbuf, sc, outbuf, part, rs, zs, zr, val, wgt, gb, left, right,
    rp, r1, r1s, r2, r2s, r3,
    load_sem, x_sem, xsend_sem, rs_sem, rssend_sem, z_sem, zsend_sem, ag_sem, agsend_sem,
    out_sem, r_sem, rsend_sem,
):
    s = lax.axis_index("section")
    d = lax.axis_index("dp")
    p = lax.rem(d, PLANE)
    zl = d // PLANE
    core = lax.rem(d, 2)
    y = p // 2
    zpeer = (s, lax.rem(d + PLANE, 2 * PLANE))
    cpeer = (s, d + 1 - 2 * core)

    def plane_peer(offset):
        return (s, zl * PLANE + lax.rem(p + offset, PLANE))

    load_wv = pltpu.make_async_copy(wv_hbm, wv, load_sem.at[0])
    load_wo = pltpu.make_async_copy(wo_hbm, wo, load_sem.at[1])
    load_cot = pltpu.make_async_copy(cot_hbm, cot, load_sem.at[2])
    load_left = pltpu.make_async_copy(left_old_hbm, left, load_sem.at[3])
    load_right = pltpu.make_async_copy(right_old_hbm, right, load_sem.at[4])
    load_wv.start()

    @pl.when(s == 0)
    def _():
        def body(c, carry):
            pltpu.make_async_copy(x_hbm.at[c], xbuf.at[c], x_sem.at[c]).start()
            return carry

        lax.fori_loop(0, NC, body, 0)

    load_wo.start()
    load_cot.start()
    load_left.start()
    load_right.start()

    barrier = pltpu.get_barrier_semaphore()
    for offset in range(1, PLANE):
        pl.semaphore_signal(barrier, inc=1, device_id=plane_peer(offset), device_id_type=MESH)
    pl.semaphore_signal(barrier, inc=1, device_id=zpeer, device_id_type=MESH)

    for step in (1, 7):
        pl.semaphore_signal(
            barrier, inc=1, device_id=(lax.rem(s + step, 8), d), device_id_type=MESH
        )
    pl.semaphore_wait(barrier, PLANE + 2)
    load_wv.wait()
    load_wo.wait()
    load_cot.wait()

    def rs_copy(c, offset):
        return pltpu.make_async_remote_copy(
            src_ref=part.at[c, lax.rem(p + offset, PLANE)],
            dst_ref=rs.at[c, offset - 1],
            send_sem=rssend_sem.at[c],
            recv_sem=rs_sem.at[c],
            device_id=plane_peer(offset),
            device_id_type=MESH,
        )

    def z_copy(c):
        return pltpu.make_async_remote_copy(
            src_ref=zs.at[c], dst_ref=zr.at[c], send_sem=zsend_sem.at[c], recv_sem=z_sem.at[c],
            device_id=zpeer, device_id_type=MESH,
        )

    def ag_copy(c, offset):
        return pltpu.make_async_remote_copy(
            src_ref=val.at[c, p], dst_ref=val.at[c, p], send_sem=agsend_sem.at[c], recv_sem=ag_sem.at[c],
            device_id=plane_peer(offset), device_id_type=MESH,
        )

    def x_copy(c):
        return pltpu.make_async_remote_copy(
            src_ref=outbuf.at[c], dst_ref=xbuf.at[c], send_sem=xsend_sem.at[c], recv_sem=x_sem.at[c],
            device_id=(s + 1, d), device_id_type=MESH,
        )

    def out_copy(c):
        return pltpu.make_async_copy(outbuf.at[c], out_hbm.at[c], out_sem.at[c])

    def tick(k, carry):
        @pl.when(k < NC)
        def _():
            c = k
            pltpu.make_async_copy(x_hbm.at[c], xbuf.at[c], x_sem.at[c]).wait()
            floats = xbuf[c].astype(F32)
            scaled = (floats * gain_ref[...].astype(F32)).astype(BF16)
            sc[pl.ds(pl.multiple_of(c * T, T), T), :] = scaled
            squares = jnp.sum(floats * floats, axis=1, keepdims=True)
            product = jnp.dot(scaled, wv[...], preferred_element_type=F32)
            both = with_pair(product, squares)
            part[c] = both.reshape(PLANE, OWN, EXT).astype(BF16)
            for offset in range(1, PLANE):
                rs_copy(c, offset).start()

        @pl.when((k >= 1) & (k <= NC))
        def _():
            c = k - 1
            pltpu.make_async_copy(rs.at[c], rs.at[c], rs_sem.at[c]).wait()
            total = part[c, p].astype(F32)
            for j in range(PLANE - 1):
                total += rs[c, j].astype(F32)
            mine = with_pair(total[:, :KV], pair_of(total)).astype(BF16)
            zs[c] = mine
            z_copy(c).start()
            pltpu.make_async_copy(zr.at[c], zr.at[c], z_sem.at[c]).wait()
            total = zs[c].astype(F32) + zr[c].astype(F32)
            inv = lax.rsqrt(pair_of(total) / D + 0.25)
            val[c, p] = with_pair(inv * total[:, :KV], inv).astype(BF16)
            for offset in range(1, PLANE):
                ag_copy(c, offset).start()

        @pl.when(k >= 2)
        def _():
            c = k - 2
            pltpu.make_async_copy(rs.at[c], rs.at[c], ag_sem.at[c]).wait()
            rows = pl.ds(pl.multiple_of(c * T, T), T)
            both = val[c].astype(F32).reshape(T, EXT)
            values = both[:, :KV].astype(BF16)
            result = xbuf[c].astype(F32) + jnp.dot(values, wo[...], preferred_element_type=F32)
            outbuf[c] = result.astype(BF16)

            @pl.when(s < 7)
            def _():
                x_copy(c).start()

            out_copy(c).start()
            wgt[rows, :] = (pair_of(both) * cot[rows, :].astype(F32)).astype(BF16)

        return carry

    lax.fori_loop(0, NC + 2, tick, 0)

    over_rows = (((0,), (0,)), ((), ()))
    over_cols = (((1,), (1,)), ((), ()))
    STEP = 256

    def block(i):
        return pl.ds(pl.multiple_of(i * STEP, STEP), STEP)

    def grad_block(i, carry):
        gb[block(i), :] = lax.dot_general(
            sc[:, block(i)], wgt[...], over_rows, preferred_element_type=F32
        ).astype(BF16)
        return carry

    lax.fori_loop(0, W // STEP, grad_block, 0)

    def right_block(i, carry):
        rows = lax.dot_general(gb[:, block(i)], gb[...], over_rows, preferred_element_type=F32).astype(BF16)
        for j in range(4):
            rp[j % 2, 2 * lax.rem(i, 2) + j // 2, i // 2] = rows[64 * j : 64 * (j + 1), :]
        return carry

    lax.fori_loop(0, KV // STEP, right_block, 0)

    core_copy = pltpu.make_async_remote_copy(
        src_ref=rp.at[1 - core], dst_ref=r1, send_sem=rsend_sem.at[0], recv_sem=r_sem.at[0],
        device_id=cpeer, device_id_type=MESH,
    )
    core_copy.start()

    load_left.wait()
    load_right.wait()

    def left_block(i, carry):
        add = lax.dot_general(gb[block(i), :], gb[...], over_cols, preferred_element_type=F32)
        left[block(i), :] = left[block(i), :] + add * (1.0 / 1024)
        return carry

    lax.fori_loop(0, 2, left_block, 0)
    core_copy.wait()
    r1s[...] = (rp[core].astype(F32) + r1[...].astype(F32)).astype(BF16)

    def y_copy(offset):
        return pltpu.make_async_remote_copy(
            src_ref=r1s.at[lax.rem(y + offset, Y)], dst_ref=r2.at[offset - 1],
            send_sem=rsend_sem.at[1], recv_sem=r_sem.at[1],
            device_id=(s, zl * PLANE + lax.rem(y + offset, Y) * 2 + core), device_id_type=MESH,
        )

    for offset in range(1, Y):
        y_copy(offset).start()
    lax.fori_loop(2, 4, left_block, 0)
    left_copy = pltpu.make_async_copy(left, left_hbm, load_sem.at[3])
    left_copy.start()
    pltpu.make_async_copy(r2, r2, r_sem.at[1]).wait()
    summed = r1s[y].astype(F32)
    for j in range(Y - 1):
        summed += r2[j].astype(F32)
    r2s[...] = summed.astype(BF16)
    last_copy = pltpu.make_async_remote_copy(
        src_ref=r2s.at[1 - zl], dst_ref=r3, send_sem=rsend_sem.at[2], recv_sem=r_sem.at[2],
        device_id=zpeer, device_id_type=MESH,
    )
    last_copy.start()
    last_copy.wait()
    right[...] = right[...] + (r2s[zl].astype(F32) + r3[...].astype(F32)) * (1.0 / D)
    right_copy = pltpu.make_async_copy(right, right_hbm, load_sem.at[4])
    right_copy.start()

    pltpu.make_async_copy(r2, r2, rsend_sem.at[1]).wait()

    def drain(c, carry):
        pltpu.make_async_copy(rs.at[c], rs.at[c], rssend_sem.at[c]).wait()
        pltpu.make_async_copy(rs.at[c], rs.at[c], agsend_sem.at[c]).wait()
        pltpu.make_async_copy(zs.at[c], zs.at[c], zsend_sem.at[c]).wait()
        out_copy(c).wait()

        @pl.when(s < 7)
        def _():
            pltpu.make_async_copy(outbuf.at[c], outbuf.at[c], xsend_sem.at[c]).wait()

        return carry

    lax.fori_loop(0, NC, drain, 0)
    left_copy.wait()
    right_copy.wait()


def on_device(inputs, cotangent, norm_gain, value_weight, output_weight, left_old, right_old):
    any_space = pl.BlockSpec(memory_space=pl.ANY)
    vmem = pl.BlockSpec(memory_space=pltpu.VMEM)
    dma = pltpu.SemaphoreType.DMA
    out, left, right = pl.pallas_call(
        kernel,
        out_shape=(
            jax.ShapeDtypeStruct((NC, T, W), BF16),
            jax.ShapeDtypeStruct((W, W), F32),
            jax.ShapeDtypeStruct((64, KV), F32),
        ),
        in_specs=[any_space, any_space, vmem, any_space, any_space, any_space, any_space],
        out_specs=(any_space, any_space, any_space),
        scratch_shapes=[
            pltpu.VMEM((W, KV), BF16),
            pltpu.VMEM((KV, W), BF16),
            pltpu.VMEM((ROWS, KV), BF16),
            pltpu.VMEM((NC, T, W), BF16),
            pltpu.VMEM((ROWS, W), BF16),
            pltpu.VMEM((NC, T, W), BF16),
            pltpu.VMEM((NC, PLANE, OWN, EXT), BF16),
            pltpu.VMEM((NC, PLANE - 1, OWN, EXT), BF16),
            pltpu.VMEM((NC, OWN, EXT), BF16),
            pltpu.VMEM((NC, OWN, EXT), BF16),
            pltpu.VMEM((NC, PLANE, OWN, EXT), BF16),
            pltpu.VMEM((ROWS, KV), BF16),
            pltpu.VMEM((W, KV), BF16),
            pltpu.VMEM((W, W), F32),
            pltpu.VMEM((64, KV), F32),
            pltpu.VMEM((2, Y, 2, 64, KV), BF16),
            pltpu.VMEM((Y, 2, 64, KV), BF16),
            pltpu.VMEM((Y, 2, 64, KV), BF16),
            pltpu.VMEM((Y - 1, 2, 64, KV), BF16),
            pltpu.VMEM((2, 64, KV), BF16),
            pltpu.VMEM((64, KV), BF16),
            dma((5,)),
            dma((NC,)),
            dma((NC,)),
            dma((NC,)),
            dma((NC,)),
            dma((NC,)),
            dma((NC,)),
            dma((NC,)),
            dma((NC,)),
            dma((NC,)),
            dma((3,)),
            dma((3,)),
        ],
        compiler_params=pltpu.CompilerParams(
            collective_id=0, has_side_effects=True, vmem_limit_bytes=60 * 1024 * 1024
        ),
    )(
        inputs.reshape(NC, T, W),
        cotangent.reshape(ROWS, KV),
        norm_gain,
        value_weight[0],
        output_weight[0],
        left_old[0, 0],
        right_old[0],
    )
    return out.reshape(1, 8, 128, W), left[None, None], right[None]


def solution(mesh):
    placed = (
        P(None, None, "dp"),
        P("section", None, None, None),
        P("section", "dp"),
        P("section", "dp", None),
        P("section", None, "dp"),
        P("section", "dp", None, None),
        P("section", "dp", None),
    )
    return jax.shard_map(
        on_device,
        mesh=mesh,
        in_specs=placed,
        out_specs=(
            P("section", None, None, "dp"),
            P("section", "dp", None, None),
            P("section", "dp", None),
        ),
        check_vma=False,
    )
```

```python
import jax
import jax.numpy as jnp
from jax import lax
from jax.experimental import pallas as pl
from jax.experimental.pallas import tpu as pltpu
from jax.sharding import PartitionSpec as P

MESH = pl.DeviceIdType.MESH
F32 = jnp.float32
BF16 = jnp.bfloat16

D = 16384
W = 1024
KV = 1024
ROWS = 1024
T = 32
NC = ROWS // 2 // T
Y = 4
OWN = T // Y
EXT = KV + 128
LAG2, LAG3, LAG4 = 1, 1, 2
ORDER = (1, 2, 3, 4)


def with_pair(rows, scalar):
    high = scalar.astype(BF16).astype(F32)
    low = scalar - high
    lane = lax.broadcasted_iota(jnp.int32, (rows.shape[0], 128), 1)
    pair = jnp.where(lane < 64, high, low)
    return jnp.concatenate([rows, pair], axis=1)


def pair_of(ext):
    return ext[:, KV : KV + 1] + ext[:, KV + 64 : KV + 65]


def kernel(
    x_hbm, cot_hbm, gain_ref, wv_hbm, wo_hbm, left_old_hbm, right_old_hbm,
    out_hbm, left_hbm, right_hbm,
    wv, wo, gain, cot, xbuf, sc, sct, outbuf, part, rs, zs, zr, val, wgt, gb, left, right,
    rpa, rpb, r1a, r1b, r2a, r2b, ta, tb, r3a, r3b,
    load_sem, x_sem, rs_sem, z_sem, ag_sem, out_sem, give_sem, send_sem, r_sem, rsend_sem,
):
    s = lax.axis_index("section")
    d = lax.axis_index("dp")
    zl = d // 8
    core = lax.rem(d, 2)
    y = lax.rem(d, 8) // 2
    zpeer = (s, lax.rem(d + 8, 16))
    cpeer = (s, d + 1 - 2 * core)

    def y_peer(offset):
        return (s, zl * 8 + lax.rem(y + offset, Y) * 2 + core)

    def rows_of(c):
        return pl.ds(pl.multiple_of(core * (ROWS // 2) + c * T, T), T)

    def remote(src, dst, send, recv, device):
        return pltpu.make_async_remote_copy(
            src_ref=src, dst_ref=dst, send_sem=send, recv_sem=recv, device_id=device, device_id_type=MESH
        )

    def wait_for(ref, sem):
        pltpu.make_async_copy(ref, ref, sem).wait()

    @pl.when(s == 0)
    def _():
        def body(c, carry):
            pltpu.make_async_copy(x_hbm.at[core, c], xbuf.at[c, core], x_sem.at[c]).start()
            return carry

        lax.fori_loop(0, NC, body, 0)

    pltpu.make_async_copy(wv_hbm, wv.at[core], load_sem.at[0]).start()
    pltpu.make_async_copy(wo_hbm, wo.at[core], load_sem.at[1]).start()
    load_cot = pltpu.make_async_copy(cot_hbm.at[core], cot, load_sem.at[2])
    load_left = pltpu.make_async_copy(left_old_hbm, left, load_sem.at[3])
    load_right = pltpu.make_async_copy(right_old_hbm, right, load_sem.at[4])
    pltpu.make_async_copy(gain_ref, gain.at[core], load_sem.at[5]).start()
    load_cot.start()
    load_left.start()
    load_right.start()

    barrier = pltpu.get_barrier_semaphore()
    for offset in range(1, Y):
        pl.semaphore_signal(barrier, inc=1, device_id=y_peer(offset), device_id_type=MESH)
    for peer in (zpeer, cpeer, (lax.rem(s + 1, 8), d), (lax.rem(s + 7, 8), d)):
        pl.semaphore_signal(barrier, inc=1, device_id=peer, device_id_type=MESH)
    pl.semaphore_wait(barrier, Y + 3)

    @pl.when(s == 0)
    def _():
        remote(x_hbm.at[1 - core, 0], xbuf.at[0, core], send_sem.at[0], x_sem.at[0], cpeer).start()

    remote(gain_ref, gain.at[core], send_sem.at[1], load_sem.at[5], cpeer).start()
    remote(wv_hbm, wv.at[core], send_sem.at[2], load_sem.at[0], cpeer).start()

    @pl.when(s == 0)
    def _():
        def body(c, carry):
            remote(x_hbm.at[1 - core, c], xbuf.at[c, core], send_sem.at[0], x_sem.at[c], cpeer).start()
            return carry

        lax.fori_loop(1, NC, body, 0)

    remote(wo_hbm, wo.at[core], send_sem.at[3], load_sem.at[1], cpeer).start()
    wait_for(gain, load_sem.at[5])
    wait_for(wv, load_sem.at[0])

    def rs_copy(c, offset):
        return remote(
            part.at[c, lax.rem(y + offset, Y)], rs.at[c, offset - 1], send_sem.at[4], rs_sem.at[c], y_peer(offset)
        )

    def ag_copy(c, offset):
        return remote(val.at[c, y], val.at[c, y], send_sem.at[5], ag_sem.at[c], y_peer(offset))

    def stage1(c):
        wait_for(xbuf.at[c], x_sem.at[c])
        product = None
        squares = None
        scaled = []
        for h in range(2):
            floats = xbuf[c, h].astype(F32)
            scaled.append((floats * gain[h].astype(F32)).astype(BF16))
            sums = jnp.sum(floats * floats, axis=1, keepdims=True)
            squares = sums if h == 0 else squares + sums
            dot = jnp.dot(scaled[h], wv[h], preferred_element_type=F32)
            product = dot if h == 0 else product + dot
        both = with_pair(product, squares)
        part[c] = both.reshape(Y, OWN, EXT).astype(BF16)
        for offset in range(1, Y):
            rs_copy(c, offset).start()
        sc[rows_of(c), :] = jnp.where(core == 0, scaled[0], scaled[1])
        sct[c] = jnp.where(core == 0, scaled[1], scaled[0])
        remote(sct.at[c], sc.at[rows_of(c)], send_sem.at[6], give_sem.at[0], cpeer).start()

    def stage2(c):
        wait_for(rs.at[c], rs_sem.at[c])
        total = part[c, y].astype(F32)
        for j in range(Y - 1):
            total += rs[c, j].astype(F32)
        zs[c] = with_pair(total[:, :KV], pair_of(total)).astype(BF16)
        remote(zs.at[c], zr.at[c], send_sem.at[7], z_sem.at[c], zpeer).start()

    def stage3(c):
        wait_for(zr.at[c], z_sem.at[c])
        total = zs[c].astype(F32) + zr[c].astype(F32)
        inv = lax.rsqrt(pair_of(total) / D + 0.25)
        val[c, y] = with_pair(inv * total[:, :KV], inv).astype(BF16)
        for offset in range(1, Y):
            ag_copy(c, offset).start()

    def stage4(c):
        wait_for(rs.at[c], ag_sem.at[c])
        both = val[c].astype(F32).reshape(T, EXT)
        values = both[:, :KV].astype(BF16)
        for h in range(2):
            result = xbuf[c, h].astype(F32) + jnp.dot(values, wo[h], preferred_element_type=F32)
            outbuf[c, h] = result.astype(BF16)

        @pl.when(s < 7)
        def _():
            remote(outbuf.at[c], xbuf.at[c], send_sem.at[8], x_sem.at[c], (s + 1, d)).start()

        wgt[rows_of(c), :] = (pair_of(both) * cot[c].astype(F32)).astype(BF16)
        remote(wgt.at[rows_of(c)], wgt.at[rows_of(c)], send_sem.at[9], give_sem.at[1], cpeer).start()
        pltpu.make_async_copy(outbuf.at[c, core], out_hbm.at[core, c], out_sem.at[0]).start()
        remote(outbuf.at[c, 1 - core], out_hbm.at[core, c], send_sem.at[10], out_sem.at[1], cpeer).start()

    stages = {1: (stage1, 0), 2: (stage2, LAG2), 3: (stage3, LAG3), 4: (stage4, LAG4)}

    def tick(k, carry):
        @pl.when(k == LAG4)
        def _():
            wait_for(wo, load_sem.at[1])
            load_cot.wait()

        for which in ORDER:
            stage, lag = stages[which]

            @pl.when((k >= lag) & (k < NC + lag))
            def _(stage=stage, lag=lag):
                stage(k - lag)

        return carry

    lax.fori_loop(0, NC + LAG4, tick, 0)

    over_rows = (((0,), (0,)), ((), ()))
    over_cols = (((1,), (1,)), ((), ()))
    STEP = 256

    def block(i):
        return pl.ds(pl.multiple_of(i * STEP, STEP), STEP)

    other = pl.ds(pl.multiple_of((1 - core) * (ROWS // 2), ROWS // 2), ROWS // 2)
    wait_for(sc.at[other], give_sem.at[0])
    wait_for(wgt.at[other], give_sem.at[1])

    def grad_block(i, carry):
        gb[block(i), :] = lax.dot_general(
            sc[:, block(i)], wgt[...], over_rows, preferred_element_type=F32
        ).astype(BF16)
        return carry

    lax.fori_loop(0, W // STEP, grad_block, 0)

    half = KV // 2

    def right_rows(i, h):
        return lax.dot_general(
            gb[:, block(i)], gb[:, h * half : (h + 1) * half], over_rows, preferred_element_type=F32
        ).astype(BF16)

    def right_b(i, carry):
        rows = right_rows(i, 1)
        for j in range(4):
            rpb[j % 2, i // 2, 2 * lax.rem(i, 2) + j // 2] = rows[64 * j : 64 * (j + 1), :]
        return carry

    def right_a(i, carry):
        rows = right_rows(i, 0)
        for j in range(4):
            rpa[j % 2, 2 * lax.rem(i, 2) + j // 2, i // 2] = rows[64 * j : 64 * (j + 1), :]
        return carry

    core_b = remote(rpb.at[1 - core], r1b, rsend_sem.at[0], r_sem.at[0], cpeer)
    core_a = remote(rpa.at[1 - core], r1a, rsend_sem.at[1], r_sem.at[1], cpeer)
    lax.fori_loop(0, KV // STEP, right_b, 0)
    core_b.start()
    lax.fori_loop(0, KV // STEP, right_a, 0)
    core_a.start()

    def left_block(i, carry):
        add = lax.dot_general(gb[block(i), :], gb[...], over_cols, preferred_element_type=F32)
        left[block(i), :] = left[block(i), :] + add * (1.0 / 1024)
        return carry

    core_b.wait()
    r1b[...] = (rpb[core].astype(F32) + r1b[...].astype(F32)).astype(BF16)
    z_b = remote(r1b.at[1 - zl], r2b, rsend_sem.at[2], r_sem.at[2], zpeer)
    z_b.start()
    core_a.wait()
    r1a[...] = (rpa[core].astype(F32) + r1a[...].astype(F32)).astype(BF16)
    for offset in range(1, Y):
        remote(
            r1a.at[lax.rem(y + offset, Y)], r2a.at[offset - 1], rsend_sem.at[3], r_sem.at[3], y_peer(offset)
        ).start()
    load_left.wait()
    load_right.wait()
    lax.fori_loop(0, W // STEP, left_block, 0)
    left_copy = pltpu.make_async_copy(left, left_hbm, load_sem.at[3])
    left_copy.start()
    z_b.wait()
    tb[...] = (r1b[zl].astype(F32) + r2b[...].astype(F32)).astype(BF16)
    for offset in range(1, Y):
        remote(
            tb.at[lax.rem(y + offset, Y)], r3b.at[offset - 1], rsend_sem.at[4], r_sem.at[4], y_peer(offset)
        ).start()
    wait_for(r2a, r_sem.at[3])
    summed = r1a[y].astype(F32)
    for j in range(Y - 1):
        summed += r2a[j].astype(F32)
    ta[...] = summed.astype(BF16)
    z_a = remote(ta.at[1 - zl], r3a, rsend_sem.at[5], r_sem.at[5], zpeer)
    z_a.start()
    wait_for(r3b, r_sem.at[4])
    summed = tb[y].astype(F32)
    for j in range(Y - 1):
        summed += r3b[j].astype(F32)
    right[:, half:] = right[:, half:] + summed * (1.0 / D)
    z_a.wait()
    right[:, :half] = right[:, :half] + (ta[zl].astype(F32) + r3a[...].astype(F32)) * (1.0 / D)
    right_copy = pltpu.make_async_copy(right, right_hbm, load_sem.at[4])
    right_copy.start()

    wait_for(r2a, rsend_sem.at[3])
    wait_for(r3b, rsend_sem.at[4])
    wait_for(gain.at[0], send_sem.at[1])
    wait_for(wv.at[0], send_sem.at[2])
    wait_for(wo.at[0], send_sem.at[3])
    wait_for(rs, send_sem.at[4])
    wait_for(rs, send_sem.at[5])
    wait_for(sct, send_sem.at[6])
    wait_for(zs, send_sem.at[7])
    wait_for(wgt.at[other], send_sem.at[9])
    wait_for(sct, send_sem.at[10])
    wait_for(sct, out_sem.at[0])
    wait_for(sct, out_sem.at[1])

    @pl.when(s == 0)
    def _():
        wait_for(sct, send_sem.at[0])

    @pl.when(s < 7)
    def _():
        wait_for(outbuf, send_sem.at[8])

    left_copy.wait()
    right_copy.wait()


def on_device(inputs, cotangent, norm_gain, value_weight, output_weight, left_old, right_old):
    any_space = pl.BlockSpec(memory_space=pl.ANY)
    dma = pltpu.SemaphoreType.DMA
    out, left, right = pl.pallas_call(
        kernel,
        out_shape=(
            jax.ShapeDtypeStruct((2, NC, T, W), BF16),
            jax.ShapeDtypeStruct((W, W), F32),
            jax.ShapeDtypeStruct((64, KV), F32),
        ),
        in_specs=[any_space] * 7,
        out_specs=(any_space, any_space, any_space),
        scratch_shapes=[
            pltpu.VMEM((2, W, KV), BF16),
            pltpu.VMEM((2, KV, W), BF16),
            pltpu.VMEM((2, 1, W), BF16),
            pltpu.VMEM((NC, T, KV), BF16),
            pltpu.VMEM((NC, 2, T, W), BF16),
            pltpu.VMEM((ROWS, W), BF16),
            pltpu.VMEM((NC, T, W), BF16),
            pltpu.VMEM((NC, 2, T, W), BF16),
            pltpu.VMEM((NC, Y, OWN, EXT), BF16),
            pltpu.VMEM((NC, Y - 1, OWN, EXT), BF16),
            pltpu.VMEM((NC, OWN, EXT), BF16),
            pltpu.VMEM((NC, OWN, EXT), BF16),
            pltpu.VMEM((NC, Y, OWN, EXT), BF16),
            pltpu.VMEM((ROWS, KV), BF16),
            pltpu.VMEM((W, KV), BF16),
            pltpu.VMEM((W, W), F32),
            pltpu.VMEM((64, KV), F32),
            pltpu.VMEM((2, Y, 2, 64, KV // 2), BF16),
            pltpu.VMEM((2, 2, Y, 64, KV // 2), BF16),
            pltpu.VMEM((Y, 2, 64, KV // 2), BF16),
            pltpu.VMEM((2, Y, 64, KV // 2), BF16),
            pltpu.VMEM((Y - 1, 2, 64, KV // 2), BF16),
            pltpu.VMEM((Y, 64, KV // 2), BF16),
            pltpu.VMEM((2, 64, KV // 2), BF16),
            pltpu.VMEM((Y, 64, KV // 2), BF16),
            pltpu.VMEM((64, KV // 2), BF16),
            pltpu.VMEM((Y - 1, 64, KV // 2), BF16),
            dma((6,)),
            dma((NC,)),
            dma((NC,)),
            dma((NC,)),
            dma((NC,)),
            dma((2,)),
            dma((2,)),
            dma((11,)),
            dma((6,)),
            dma((6,)),
        ],
        compiler_params=pltpu.CompilerParams(
            collective_id=0, has_side_effects=True, vmem_limit_bytes=60 * 1024 * 1024
        ),
    )(
        inputs.reshape(2, NC, T, W),
        cotangent.reshape(2, NC, T, KV),
        norm_gain,
        value_weight[0],
        output_weight[0],
        left_old[0, 0],
        right_old[0],
    )
    return out.reshape(1, 8, 128, W), left[None, None], right[None]


def solution(mesh):
    placed = (
        P(None, None, "dp"),
        P("section", None, None, None),
        P("section", "dp"),
        P("section", "dp", None),
        P("section", None, "dp"),
        P("section", "dp", None, None),
        P("section", "dp", None),
    )
    return jax.shard_map(
        on_device,
        mesh=mesh,
        in_specs=placed,
        out_specs=(
            P("section", None, None, "dp"),
            P("section", "dp", None, None),
            P("section", "dp", None),
        ),
        check_vma=False,
    )
```

```python
import jax
import jax.numpy as jnp
from jax import lax
from jax.experimental import pallas as pl
from jax.experimental.pallas import tpu as pltpu
from jax.sharding import PartitionSpec as P

MESH = pl.DeviceIdType.MESH
F32 = jnp.float32
BF16 = jnp.bfloat16

D = 16384
W = 1024
KV = 1024
ROWS = 1024
T = 32
NC = ROWS // 2 // T
Y = 4
OWN = T // Y
EXT = KV + 128
LAG2, LAG3, LAG4 = 1, 2, 3
ORDER = (0, 1, 2, 3, 4)
LAG0 = -1
LATE = 4
PIECES = 4


def with_pair(rows, scalar):
    high = scalar.astype(BF16).astype(F32)
    low = scalar - high
    lane = lax.broadcasted_iota(jnp.int32, (rows.shape[0], 128), 1)
    pair = jnp.where(lane < 64, high, low)
    return jnp.concatenate([rows, pair], axis=1)


def pair_of(ext):
    return ext[:, KV : KV + 1] + ext[:, KV + 64 : KV + 65]


def kernel(
    x_hbm, cot_hbm, gain_ref, wv_hbm, wo_hbm, left_old_hbm, right_old_hbm,
    out_hbm, left_hbm, right_hbm,
    wv, wo, wop, gain, cot, xbuf, vin, sc, sct, outbuf, part, rs, zs, zr, val, wgt, gb, left, right,
    rpa, rpb, r1a, r1b, r2a, r2b, ta, tb, r3a, r3b,
    load_sem, x_sem, rs_sem, z_sem, ag_sem, out_sem, give_sem, v_sem, v2_sem, pre_sem, send_sem, r_sem, rsend_sem,
):
    s = lax.axis_index("section")
    d = lax.axis_index("dp")
    zl = d // 8
    core = lax.rem(d, 2)
    y = lax.rem(d, 8) // 2
    odd = lax.rem(s, 2) == 1
    zpeer = (s, lax.rem(d + 8, 16))
    cpeer = (s, d + 1 - 2 * core)

    def y_peer(offset):
        return (s, zl * 8 + lax.rem(y + offset, Y) * 2 + core)

    def rows_of(c):
        return pl.ds(pl.multiple_of(core * (ROWS // 2) + c * T, T), T)

    def remote(src, dst, send, recv, device):
        return pltpu.make_async_remote_copy(
            src_ref=src, dst_ref=dst, send_sem=send, recv_sem=recv, device_id=device, device_id_type=MESH
        )

    def wait_for(ref, sem):
        pltpu.make_async_copy(ref, ref, sem).wait()

    @pl.when(s == 0)
    def _():
        def body(c, carry):
            pltpu.make_async_copy(x_hbm.at[core, c], xbuf.at[c, core], x_sem.at[c]).start()
            return carry

        lax.fori_loop(0, NC, body, 0)

    pltpu.make_async_copy(wv_hbm, wv.at[core], load_sem.at[0]).start()
    pltpu.make_async_copy(wo_hbm, wo.at[core], load_sem.at[1]).start()
    load_cot = pltpu.make_async_copy(cot_hbm.at[core], cot, load_sem.at[2])
    load_left = pltpu.make_async_copy(left_old_hbm, left, load_sem.at[3])
    load_right = pltpu.make_async_copy(right_old_hbm, right, load_sem.at[4])
    pltpu.make_async_copy(gain_ref, gain.at[core], load_sem.at[5]).start()
    load_cot.start()
    load_left.start()
    load_right.start()

    barrier = pltpu.get_barrier_semaphore()
    for offset in range(1, Y):
        pl.semaphore_signal(barrier, inc=1, device_id=y_peer(offset), device_id_type=MESH)
    for step in (1, 7):
        for offset in range(Y):
            peer = (lax.rem(s + step, 8), y_peer(offset)[1])
            pl.semaphore_signal(barrier, inc=1, device_id=peer, device_id_type=MESH)
    for peer in (zpeer, cpeer, (lax.rem(s + 2, 8), d), (lax.rem(s + 6, 8), d)):
        pl.semaphore_signal(barrier, inc=1, device_id=peer, device_id_type=MESH)
    pl.semaphore_wait(barrier, Y - 1 + 2 * Y + 4)

    @pl.when(s == 0)
    def _():
        remote(x_hbm.at[1 - core, 0], xbuf.at[0, core], send_sem.at[0], x_sem.at[0], cpeer).start()

    remote(gain_ref, gain.at[core], send_sem.at[1], load_sem.at[5], cpeer).start()
    remote(wv_hbm, wv.at[core], send_sem.at[2], load_sem.at[0], cpeer).start()

    @pl.when(s == 0)
    def _():
        def body(c, carry):
            remote(x_hbm.at[1 - core, c], xbuf.at[c, core], send_sem.at[0], x_sem.at[c], cpeer).start()
            return carry

        lax.fori_loop(1, NC, body, 0)

    remote(wo_hbm, wo.at[core], send_sem.at[3], load_sem.at[1], cpeer).start()

    def piece(i):
        return pl.ds(i * (KV // PIECES), KV // PIECES)

    @pl.when((s >= LATE - 1) & (s < 7))
    def _():
        for i in range(PIECES):
            remote(
                wo_hbm.at[piece(i)], wop.at[core, piece(i)], send_sem.at[11], pre_sem.at[i], (s + 1, d)
            ).start()

    @pl.when(s >= LATE)
    def _():
        for i in range(PIECES):
            ours = wop.at[core, piece(i)]
            wait_for(ours, pre_sem.at[i])
            remote(ours, ours, send_sem.at[12], pre_sem.at[PIECES], cpeer).start()
        wait_for(wop.at[0], pre_sem.at[PIECES])

    wait_for(gain, load_sem.at[5])
    wait_for(wv, load_sem.at[0])

    def rs_copy(c, offset):
        return remote(
            part.at[c, lax.rem(y + offset, Y)], rs.at[c, offset - 1], send_sem.at[4], rs_sem.at[c], y_peer(offset)
        )

    def ag_copy(c, offset):
        return remote(val.at[c, y], val.at[c, y], send_sem.at[5], ag_sem.at[c], y_peer(offset))

    def stage0(c):
        @pl.when((s >= LATE) & jnp.logical_not(odd))
        def _():
            wait_for(vin.at[c, y], v_sem.at[c])
            for offset in range(1, Y):
                remote(vin.at[c, y], vin.at[c, y], send_sem.at[15], v2_sem.at[c], y_peer(offset)).start()

    def stage1(c):
        wait_for(xbuf.at[c], x_sem.at[c])

        @pl.when(s >= LATE)
        def _():
            @pl.when(odd)
            def _():
                wait_for(vin.at[c], v_sem.at[c])

            @pl.when(jnp.logical_not(odd))
            def _():
                wait_for(rs.at[c], v2_sem.at[c])

            before = vin[c].astype(F32).reshape(T, EXT)[:, :KV].astype(BF16)
            for h in range(2):
                made = xbuf[c, h].astype(F32) + jnp.dot(before, wop[h], preferred_element_type=F32)
                xbuf[c, h] = made.astype(BF16)

        product = None
        squares = None
        scaled = []
        for h in range(2):
            floats = xbuf[c, h].astype(F32)
            scaled.append((floats * gain[h].astype(F32)).astype(BF16))
            sums = jnp.sum(floats * floats, axis=1, keepdims=True)
            squares = sums if h == 0 else squares + sums
            dot = jnp.dot(scaled[h], wv[h], preferred_element_type=F32)
            product = dot if h == 0 else product + dot
        both = with_pair(product, squares)
        part[c] = both.reshape(Y, OWN, EXT).astype(BF16)
        for offset in range(1, Y):
            rs_copy(c, offset).start()
        sc[rows_of(c), :] = jnp.where(core == 0, scaled[0], scaled[1])
        sct[c] = jnp.where(core == 0, scaled[1], scaled[0])
        remote(sct.at[c], sc.at[rows_of(c)], send_sem.at[6], give_sem.at[0], cpeer).start()

    def stage2(c):
        wait_for(rs.at[c], rs_sem.at[c])
        total = part[c, y].astype(F32)
        for j in range(Y - 1):
            total += rs[c, j].astype(F32)
        zs[c] = with_pair(total[:, :KV], pair_of(total)).astype(BF16)
        remote(zs.at[c], zr.at[c], send_sem.at[7], z_sem.at[c], zpeer).start()

    def stage3(c):
        wait_for(zr.at[c], z_sem.at[c])
        total = zs[c].astype(F32) + zr[c].astype(F32)
        inv = lax.rsqrt(pair_of(total) / D + 0.25)
        val[c, y] = with_pair(inv * total[:, :KV], inv).astype(BF16)

        @pl.when((s >= LATE - 1) & (s < 7))
        def _():
            remote(val.at[c, y], vin.at[c, y], send_sem.at[13], v_sem.at[c], (s + 1, d)).start()

            @pl.when(jnp.logical_not(odd))
            def _():
                for offset in range(1, Y):
                    remote(
                        val.at[c, y], vin.at[c, y], send_sem.at[15], v_sem.at[c], (s + 1, y_peer(offset)[1])
                    ).start()

        for offset in range(1, Y):
            ag_copy(c, offset).start()

    def stage4(c):
        wait_for(rs.at[c], ag_sem.at[c])
        both = val[c].astype(F32).reshape(T, EXT)
        values = both[:, :KV].astype(BF16)
        for h in range(2):
            result = xbuf[c, h].astype(F32) + jnp.dot(values, wo[h], preferred_element_type=F32)
            outbuf[c, h] = result.astype(BF16)

        @pl.when(s < LATE - 1)
        def _():
            remote(outbuf.at[c], xbuf.at[c], send_sem.at[8], x_sem.at[c], (s + 1, d)).start()

        @pl.when((s >= LATE - 2) & (s < 6))
        def _():
            remote(outbuf.at[c], xbuf.at[c], send_sem.at[14], x_sem.at[c], (s + 2, d)).start()

        wgt[rows_of(c), :] = (pair_of(both) * cot[c].astype(F32)).astype(BF16)
        remote(wgt.at[rows_of(c)], wgt.at[rows_of(c)], send_sem.at[9], give_sem.at[1], cpeer).start()
        pltpu.make_async_copy(outbuf.at[c, core], out_hbm.at[core, c], out_sem.at[0]).start()
        remote(outbuf.at[c, 1 - core], out_hbm.at[core, c], send_sem.at[10], out_sem.at[1], cpeer).start()

    stages = {0: (stage0, LAG0), 1: (stage1, 0), 2: (stage2, LAG2), 3: (stage3, LAG3), 4: (stage4, LAG4)}

    stage0(0)
    if LAG0 == -2:
        stage0(1)

    def tick(k, carry):
        @pl.when(k == LAG4)
        def _():
            wait_for(wo, load_sem.at[1])
            load_cot.wait()

        for which in ORDER:
            stage, lag = stages[which]

            @pl.when((k >= lag) & (k < NC + lag))
            def _(stage=stage, lag=lag):
                stage(k - lag)

        return carry

    lax.fori_loop(0, NC + LAG4, tick, 0)

    over_rows = (((0,), (0,)), ((), ()))
    over_cols = (((1,), (1,)), ((), ()))
    STEP = 256

    def block(i):
        return pl.ds(pl.multiple_of(i * STEP, STEP), STEP)

    other = pl.ds(pl.multiple_of((1 - core) * (ROWS // 2), ROWS // 2), ROWS // 2)
    wait_for(sc.at[other], give_sem.at[0])
    wait_for(wgt.at[other], give_sem.at[1])

    def grad_block(i, carry):
        gb[block(i), :] = lax.dot_general(
            sc[:, block(i)], wgt[...], over_rows, preferred_element_type=F32
        ).astype(BF16)
        return carry

    lax.fori_loop(0, W // STEP, grad_block, 0)

    half = KV // 2

    def right_rows(i, h):
        return lax.dot_general(
            gb[:, block(i)], gb[:, h * half : (h + 1) * half], over_rows, preferred_element_type=F32
        ).astype(BF16)

    def right_b(i, carry):
        rows = right_rows(i, 1)
        for j in range(4):
            rpb[j % 2, i // 2, 2 * lax.rem(i, 2) + j // 2] = rows[64 * j : 64 * (j + 1), :]
        return carry

    def right_a(i, carry):
        rows = right_rows(i, 0)
        for j in range(4):
            rpa[j % 2, 2 * lax.rem(i, 2) + j // 2, i // 2] = rows[64 * j : 64 * (j + 1), :]
        return carry

    core_b = remote(rpb.at[1 - core], r1b, rsend_sem.at[0], r_sem.at[0], cpeer)
    core_a = remote(rpa.at[1 - core], r1a, rsend_sem.at[1], r_sem.at[1], cpeer)
    lax.fori_loop(0, KV // STEP, right_b, 0)
    core_b.start()
    lax.fori_loop(0, KV // STEP, right_a, 0)
    core_a.start()

    def left_block(i, carry):
        add = lax.dot_general(gb[block(i), :], gb[...], over_cols, preferred_element_type=F32)
        left[block(i), :] = left[block(i), :] + add * (1.0 / 1024)
        return carry

    core_b.wait()
    r1b[...] = (rpb[core].astype(F32) + r1b[...].astype(F32)).astype(BF16)
    z_b = remote(r1b.at[1 - zl], r2b, rsend_sem.at[2], r_sem.at[2], zpeer)
    z_b.start()
    core_a.wait()
    r1a[...] = (rpa[core].astype(F32) + r1a[...].astype(F32)).astype(BF16)
    for offset in range(1, Y):
        remote(
            r1a.at[lax.rem(y + offset, Y)], r2a.at[offset - 1], rsend_sem.at[3], r_sem.at[3], y_peer(offset)
        ).start()
    load_left.wait()
    load_right.wait()
    lax.fori_loop(0, W // STEP, left_block, 0)
    left_copy = pltpu.make_async_copy(left, left_hbm, load_sem.at[3])
    left_copy.start()
    z_b.wait()
    tb[...] = (r1b[zl].astype(F32) + r2b[...].astype(F32)).astype(BF16)
    for offset in range(1, Y):
        remote(
            tb.at[lax.rem(y + offset, Y)], r3b.at[offset - 1], rsend_sem.at[4], r_sem.at[4], y_peer(offset)
        ).start()
    wait_for(r2a, r_sem.at[3])
    summed = r1a[y].astype(F32)
    for j in range(Y - 1):
        summed += r2a[j].astype(F32)
    ta[...] = summed.astype(BF16)
    z_a = remote(ta.at[1 - zl], r3a, rsend_sem.at[5], r_sem.at[5], zpeer)
    z_a.start()
    wait_for(r3b, r_sem.at[4])
    summed = tb[y].astype(F32)
    for j in range(Y - 1):
        summed += r3b[j].astype(F32)
    right[:, half:] = right[:, half:] + summed * (1.0 / D)
    z_a.wait()
    right[:, :half] = right[:, :half] + (ta[zl].astype(F32) + r3a[...].astype(F32)) * (1.0 / D)
    right_copy = pltpu.make_async_copy(right, right_hbm, load_sem.at[4])
    right_copy.start()

    wait_for(r2a, rsend_sem.at[3])
    wait_for(r3b, rsend_sem.at[4])
    wait_for(gain.at[0], send_sem.at[1])
    wait_for(wv.at[0], send_sem.at[2])
    wait_for(wo.at[0], send_sem.at[3])
    wait_for(rs, send_sem.at[4])
    wait_for(rs, send_sem.at[5])
    wait_for(sct, send_sem.at[6])
    wait_for(zs, send_sem.at[7])
    wait_for(wgt.at[other], send_sem.at[9])
    wait_for(sct, send_sem.at[10])
    wait_for(sct, out_sem.at[0])
    wait_for(sct, out_sem.at[1])

    @pl.when(s == 0)
    def _():
        wait_for(sct, send_sem.at[0])

    @pl.when(s < LATE - 1)
    def _():
        wait_for(outbuf, send_sem.at[8])

    @pl.when((s >= LATE - 2) & (s < 6))
    def _():
        wait_for(outbuf, send_sem.at[14])

    @pl.when((s >= LATE - 1) & (s < 7))
    def _():
        wait_for(wo.at[0], send_sem.at[11])
        wait_for(zs, send_sem.at[13])

    @pl.when(s >= LATE)
    def _():
        wait_for(wop.at[0], send_sem.at[12])

    @pl.when((s >= LATE) & (s < 7) & jnp.logical_not(odd))
    def _():
        wait_for(rs, send_sem.at[15])
        wait_for(rs, send_sem.at[15])

    left_copy.wait()
    right_copy.wait()


def on_device(inputs, cotangent, norm_gain, value_weight, output_weight, left_old, right_old):
    any_space = pl.BlockSpec(memory_space=pl.ANY)
    dma = pltpu.SemaphoreType.DMA
    out, left, right = pl.pallas_call(
        kernel,
        out_shape=(
            jax.ShapeDtypeStruct((2, NC, T, W), BF16),
            jax.ShapeDtypeStruct((W, W), F32),
            jax.ShapeDtypeStruct((64, KV), F32),
        ),
        in_specs=[any_space] * 7,
        out_specs=(any_space, any_space, any_space),
        scratch_shapes=[
            pltpu.VMEM((2, W, KV), BF16),
            pltpu.VMEM((2, KV, W), BF16),
            pltpu.VMEM((2, KV, W), BF16),
            pltpu.VMEM((2, 1, W), BF16),
            pltpu.VMEM((NC, T, KV), BF16),
            pltpu.VMEM((NC, 2, T, W), BF16),
            pltpu.VMEM((NC, Y, OWN, EXT), BF16),
            pltpu.VMEM((ROWS, W), BF16),
            pltpu.VMEM((NC, T, W), BF16),
            pltpu.VMEM((NC, 2, T, W), BF16),
            pltpu.VMEM((NC, Y, OWN, EXT), BF16),
            pltpu.VMEM((NC, Y - 1, OWN, EXT), BF16),
            pltpu.VMEM((NC, OWN, EXT), BF16),
            pltpu.VMEM((NC, OWN, EXT), BF16),
            pltpu.VMEM((NC, Y, OWN, EXT), BF16),
            pltpu.VMEM((ROWS, KV), BF16),
            pltpu.VMEM((W, KV), BF16),
            pltpu.VMEM((W, W), F32),
            pltpu.VMEM((64, KV), F32),
            pltpu.VMEM((2, Y, 2, 64, KV // 2), BF16),
            pltpu.VMEM((2, 2, Y, 64, KV // 2), BF16),
            pltpu.VMEM((Y, 2, 64, KV // 2), BF16),
            pltpu.VMEM((2, Y, 64, KV // 2), BF16),
            pltpu.VMEM((Y - 1, 2, 64, KV // 2), BF16),
            pltpu.VMEM((Y, 64, KV // 2), BF16),
            pltpu.VMEM((2, 64, KV // 2), BF16),
            pltpu.VMEM((Y, 64, KV // 2), BF16),
            pltpu.VMEM((64, KV // 2), BF16),
            pltpu.VMEM((Y - 1, 64, KV // 2), BF16),
            dma((6,)),
            dma((NC,)),
            dma((NC,)),
            dma((NC,)),
            dma((NC,)),
            dma((2,)),
            dma((2,)),
            dma((NC,)),
            dma((NC,)),
            dma((PIECES + 1,)),
            dma((16,)),
            dma((6,)),
            dma((6,)),
        ],
        compiler_params=pltpu.CompilerParams(
            collective_id=0, has_side_effects=True, vmem_limit_bytes=60 * 1024 * 1024
        ),
    )(
        inputs.reshape(2, NC, T, W),
        cotangent.reshape(2, NC, T, KV),
        norm_gain,
        value_weight[0],
        output_weight[0],
        left_old[0, 0],
        right_old[0],
    )
    return out.reshape(1, 8, 128, W), left[None, None], right[None]


def solution(mesh):
    placed = (
        P(None, None, "dp"),
        P("section", None, None, None),
        P("section", "dp"),
        P("section", "dp", None),
        P("section", None, "dp"),
        P("section", "dp", None, None),
        P("section", "dp", None),
    )
    return jax.shard_map(
        on_device,
        mesh=mesh,
        in_specs=placed,
        out_specs=(
            P("section", None, None, "dp"),
            P("section", "dp", None, None),
            P("section", "dp", None),
        ),
        check_vma=False,
    )
```

```python
import jax
import jax.numpy as jnp
from jax import lax
from jax.experimental import pallas as pl
from jax.experimental.pallas import tpu as pltpu
from jax.sharding import PartitionSpec as P

MESH = pl.DeviceIdType.MESH
F32 = jnp.float32
BF16 = jnp.bfloat16

D = 16384
W = 1024
KV = 1024
ROWS = 1024
T = 32
NC = ROWS // 2 // T
Y = 4
OWN = T // Y
EXT = KV + 128
LAG2, LAG3, LAG4 = 1, 2, 3
ORDER = (0, 1, 2, 3, 4)
LAG0 = -1
LATE = 4
PIECES = 4


def with_pair(rows, scalar):
    high = scalar.astype(BF16).astype(F32)
    low = scalar - high
    lane = lax.broadcasted_iota(jnp.int32, (rows.shape[0], 128), 1)
    pair = jnp.where(lane < 64, high, low)
    return jnp.concatenate([rows, pair], axis=1)


def pair_of(ext):
    return ext[:, KV : KV + 1] + ext[:, KV + 64 : KV + 65]


def kernel(
    x_hbm, cot_hbm, gain_ref, wv_hbm, wo_hbm, left_old_hbm, right_old_hbm,
    out_hbm, left_hbm, right_hbm,
    wv, wo, wop, gain, cot, xbuf, vin, sc, sct, outbuf, part, rs, zs, zr, val, wgt, gb, left, right,
    rpa, rpb, r1a, r1b, r2a, r2b, ta, tb, r3a, r3b,
    load_sem, x_sem, rs_sem, z_sem, ag_sem, out_sem, give_sem, v_sem, v2_sem, pre_sem, send_sem, r_sem, rsend_sem,
):
    s = lax.axis_index("section")
    d = lax.axis_index("dp")
    zl = d // 8
    core = lax.rem(d, 2)
    y = lax.rem(d, 8) // 2
    odd = lax.rem(s, 2) == 1
    zpeer = (s, lax.rem(d + 8, 16))
    cpeer = (s, d + 1 - 2 * core)

    def y_peer(offset):
        return (s, zl * 8 + lax.rem(y + offset, Y) * 2 + core)

    def rows_of(c):
        return pl.ds(pl.multiple_of(core * (ROWS // 2) + c * T, T), T)

    def remote(src, dst, send, recv, device):
        return pltpu.make_async_remote_copy(
            src_ref=src, dst_ref=dst, send_sem=send, recv_sem=recv, device_id=device, device_id_type=MESH
        )

    def wait_for(ref, sem):
        pltpu.make_async_copy(ref, ref, sem).wait()

    @pl.when(s == 0)
    def _():
        def body(c, carry):
            pltpu.make_async_copy(x_hbm.at[core, c], xbuf.at[c, core], x_sem.at[c]).start()
            return carry

        lax.fori_loop(0, NC, body, 0)

    pltpu.make_async_copy(wv_hbm, wv.at[core], load_sem.at[0]).start()
    pltpu.make_async_copy(wo_hbm, wo.at[core], load_sem.at[1]).start()
    load_cot = pltpu.make_async_copy(cot_hbm.at[core], cot, load_sem.at[2])
    load_left = pltpu.make_async_copy(left_old_hbm, left, load_sem.at[3])
    load_right = pltpu.make_async_copy(right_old_hbm, right, load_sem.at[4])
    pltpu.make_async_copy(gain_ref, gain.at[core], load_sem.at[5]).start()
    load_cot.start()
    load_left.start()
    load_right.start()

    barrier = pltpu.get_barrier_semaphore()
    for offset in range(1, Y):
        pl.semaphore_signal(barrier, inc=1, device_id=y_peer(offset), device_id_type=MESH)
    for step in (1, 7):
        for offset in range(Y):
            peer = (lax.rem(s + step, 8), y_peer(offset)[1])
            pl.semaphore_signal(barrier, inc=1, device_id=peer, device_id_type=MESH)
    for peer in (zpeer, cpeer, (lax.rem(s + 2, 8), d), (lax.rem(s + 6, 8), d)):
        pl.semaphore_signal(barrier, inc=1, device_id=peer, device_id_type=MESH)
    pl.semaphore_wait(barrier, Y - 1 + 2 * Y + 4)

    @pl.when(s == 0)
    def _():
        remote(x_hbm.at[1 - core, 0], xbuf.at[0, core], send_sem.at[0], x_sem.at[0], cpeer).start()

    remote(gain_ref, gain.at[core], send_sem.at[1], load_sem.at[5], cpeer).start()
    remote(wv_hbm, wv.at[core], send_sem.at[2], load_sem.at[0], cpeer).start()

    @pl.when(s == 0)
    def _():
        def body(c, carry):
            remote(x_hbm.at[1 - core, c], xbuf.at[c, core], send_sem.at[0], x_sem.at[c], cpeer).start()
            return carry

        lax.fori_loop(1, NC, body, 0)

    remote(wo_hbm, wo.at[core], send_sem.at[3], load_sem.at[1], cpeer).start()

    def piece(i):
        return pl.ds(i * (KV // PIECES), KV // PIECES)

    @pl.when((s >= LATE - 1) & (s < 7))
    def _():
        for i in range(PIECES):
            remote(
                wo_hbm.at[piece(i)], wop.at[core, piece(i)], send_sem.at[11], pre_sem.at[i], (s + 1, d)
            ).start()

    @pl.when(s >= LATE)
    def _():
        for i in range(PIECES):
            ours = wop.at[core, piece(i)]
            wait_for(ours, pre_sem.at[i])
            remote(ours, ours, send_sem.at[12], pre_sem.at[PIECES], cpeer).start()
        wait_for(wop.at[0], pre_sem.at[PIECES])

    wait_for(gain, load_sem.at[5])
    wait_for(wv, load_sem.at[0])

    def rs_copy(c, offset):
        return remote(
            part.at[c, lax.rem(y + offset, Y)], rs.at[c, offset - 1], send_sem.at[4], rs_sem.at[c], y_peer(offset)
        )

    def ag_copy(c, offset):
        return remote(val.at[c, y], val.at[c, y], send_sem.at[5], ag_sem.at[c], y_peer(offset))

    def stage0(c):
        @pl.when((s >= LATE) & jnp.logical_not(odd))
        def _():
            wait_for(vin.at[c, y], v_sem.at[c])
            for offset in range(1, Y):
                remote(vin.at[c, y], vin.at[c, y], send_sem.at[15], v2_sem.at[c], y_peer(offset)).start()

    def stage1(c):
        wait_for(xbuf.at[c], x_sem.at[c])

        @pl.when(s >= LATE)
        def _():
            @pl.when(odd)
            def _():
                wait_for(vin.at[c], v_sem.at[c])

            @pl.when(jnp.logical_not(odd))
            def _():
                wait_for(vin.at[c, pl.ds(0, Y - 1)], v2_sem.at[c])

            before = vin[c].astype(F32).reshape(T, KV).astype(BF16)
            for h in range(2):
                made = xbuf[c, h].astype(F32) + jnp.dot(before, wop[h], preferred_element_type=F32)
                xbuf[c, h] = made.astype(BF16)

        product = None
        squares = None
        scaled = []
        for h in range(2):
            floats = xbuf[c, h].astype(F32)
            scaled.append((floats * gain[h].astype(F32)).astype(BF16))
            sums = jnp.sum(floats * floats, axis=1, keepdims=True)
            squares = sums if h == 0 else squares + sums
            dot = jnp.dot(scaled[h], wv[h], preferred_element_type=F32)
            product = dot if h == 0 else product + dot
        both = with_pair(product, squares)
        part[c] = both.reshape(Y, OWN, EXT).astype(BF16)
        for offset in range(1, Y):
            rs_copy(c, offset).start()
        sc[rows_of(c), :] = jnp.where(core == 0, scaled[0], scaled[1])
        sct[c] = jnp.where(core == 0, scaled[1], scaled[0])
        remote(sct.at[c], sc.at[rows_of(c)], send_sem.at[6], give_sem.at[0], cpeer).start()

    def stage2(c):
        wait_for(rs.at[c], rs_sem.at[c])
        total = part[c, y].astype(F32)
        for j in range(Y - 1):
            total += rs[c, j].astype(F32)
        zs[c] = with_pair(total[:, :KV], pair_of(total)).astype(BF16)
        remote(zs.at[c], zr.at[c], send_sem.at[7], z_sem.at[c], zpeer).start()

    def stage3(c):
        wait_for(zr.at[c], z_sem.at[c])
        total = zs[c].astype(F32) + zr[c].astype(F32)
        inv = lax.rsqrt(pair_of(total) / D + 0.25)
        val[c, y] = with_pair(inv * total[:, :KV], inv).astype(BF16)

        @pl.when((s >= LATE - 1) & (s < 7))
        def _():
            remote(val.at[c, y, :, pl.ds(0, KV)], vin.at[c, y], send_sem.at[13], v_sem.at[c], (s + 1, d)).start()

            @pl.when(jnp.logical_not(odd))
            def _():
                for offset in range(1, Y):
                    remote(
                        val.at[c, y, :, pl.ds(0, KV)], vin.at[c, y], send_sem.at[15], v_sem.at[c], (s + 1, y_peer(offset)[1])
                    ).start()

        for offset in range(1, Y):
            ag_copy(c, offset).start()

    def stage4(c):
        wait_for(rs.at[c], ag_sem.at[c])
        both = val[c].astype(F32).reshape(T, EXT)
        values = both[:, :KV].astype(BF16)
        for h in range(2):
            result = xbuf[c, h].astype(F32) + jnp.dot(values, wo[h], preferred_element_type=F32)
            outbuf[c, h] = result.astype(BF16)

        @pl.when(s < LATE - 1)
        def _():
            remote(outbuf.at[c], xbuf.at[c], send_sem.at[8], x_sem.at[c], (s + 1, d)).start()

        @pl.when((s >= LATE - 2) & (s < 6))
        def _():
            remote(outbuf.at[c], xbuf.at[c], send_sem.at[14], x_sem.at[c], (s + 2, d)).start()

        wgt[rows_of(c), :] = (pair_of(both) * cot[c].astype(F32)).astype(BF16)
        remote(wgt.at[rows_of(c)], wgt.at[rows_of(c)], send_sem.at[9], give_sem.at[1], cpeer).start()
        pltpu.make_async_copy(outbuf.at[c, core], out_hbm.at[core, c], out_sem.at[0]).start()
        remote(outbuf.at[c, 1 - core], out_hbm.at[core, c], send_sem.at[10], out_sem.at[1], cpeer).start()

    lag4 = jnp.where(s >= LATE - 1, 4, LAG4)
    stages = {0: (stage0, LAG0), 1: (stage1, 0), 2: (stage2, LAG2), 3: (stage3, LAG3), 4: (stage4, lag4)}

    stage0(0)
    if LAG0 == -2:
        stage0(1)

    def tick(k, carry):
        @pl.when(k == LAG4)
        def _():
            wait_for(wo, load_sem.at[1])
            load_cot.wait()

        for which in ORDER:
            stage, lag = stages[which]

            @pl.when((k >= lag) & (k < NC + lag))
            def _(stage=stage, lag=lag):
                stage(k - lag)

        return carry

    lax.fori_loop(0, NC + 4, tick, 0)

    over_rows = (((0,), (0,)), ((), ()))
    over_cols = (((1,), (1,)), ((), ()))
    STEP = 256

    def block(i):
        return pl.ds(pl.multiple_of(i * STEP, STEP), STEP)

    other = pl.ds(pl.multiple_of((1 - core) * (ROWS // 2), ROWS // 2), ROWS // 2)
    wait_for(sc.at[other], give_sem.at[0])
    wait_for(wgt.at[other], give_sem.at[1])

    def grad_block(i, carry):
        gb[block(i), :] = lax.dot_general(
            sc[:, block(i)], wgt[...], over_rows, preferred_element_type=F32
        ).astype(BF16)
        return carry

    lax.fori_loop(0, W // STEP, grad_block, 0)

    half = KV // 2

    def right_rows(i, h):
        return lax.dot_general(
            gb[:, block(i)], gb[:, h * half : (h + 1) * half], over_rows, preferred_element_type=F32
        ).astype(BF16)

    def right_b(i, carry):
        rows = right_rows(i, 1)
        for j in range(4):
            rpb[j % 2, i // 2, 2 * lax.rem(i, 2) + j // 2] = rows[64 * j : 64 * (j + 1), :]
        return carry

    def right_a(i, carry):
        rows = right_rows(i, 0)
        for j in range(4):
            rpa[j % 2, 2 * lax.rem(i, 2) + j // 2, i // 2] = rows[64 * j : 64 * (j + 1), :]
        return carry

    core_b = remote(rpb.at[1 - core], r1b, rsend_sem.at[0], r_sem.at[0], cpeer)
    core_a = remote(rpa.at[1 - core], r1a, rsend_sem.at[1], r_sem.at[1], cpeer)
    lax.fori_loop(0, KV // STEP, right_b, 0)
    core_b.start()
    lax.fori_loop(0, KV // STEP, right_a, 0)
    core_a.start()

    def left_block(i, carry):
        add = lax.dot_general(gb[block(i), :], gb[...], over_cols, preferred_element_type=F32)
        left[block(i), :] = left[block(i), :] + add * (1.0 / 1024)
        return carry

    core_b.wait()
    r1b[...] = (rpb[core].astype(F32) + r1b[...].astype(F32)).astype(BF16)
    z_b = remote(r1b.at[1 - zl], r2b, rsend_sem.at[2], r_sem.at[2], zpeer)
    z_b.start()
    core_a.wait()
    r1a[...] = (rpa[core].astype(F32) + r1a[...].astype(F32)).astype(BF16)
    for offset in range(1, Y):
        remote(
            r1a.at[lax.rem(y + offset, Y)], r2a.at[offset - 1], rsend_sem.at[3], r_sem.at[3], y_peer(offset)
        ).start()
    load_left.wait()
    load_right.wait()
    lax.fori_loop(0, W // STEP, left_block, 0)
    left_copy = pltpu.make_async_copy(left, left_hbm, load_sem.at[3])
    left_copy.start()
    z_b.wait()
    tb[...] = (r1b[zl].astype(F32) + r2b[...].astype(F32)).astype(BF16)
    for offset in range(1, Y):
        remote(
            tb.at[lax.rem(y + offset, Y)], r3b.at[offset - 1], rsend_sem.at[4], r_sem.at[4], y_peer(offset)
        ).start()
    wait_for(r2a, r_sem.at[3])
    summed = r1a[y].astype(F32)
    for j in range(Y - 1):
        summed += r2a[j].astype(F32)
    ta[...] = summed.astype(BF16)
    z_a = remote(ta.at[1 - zl], r3a, rsend_sem.at[5], r_sem.at[5], zpeer)
    z_a.start()
    wait_for(r3b, r_sem.at[4])
    summed = tb[y].astype(F32)
    for j in range(Y - 1):
        summed += r3b[j].astype(F32)
    right[:, half:] = right[:, half:] + summed * (1.0 / D)
    z_a.wait()
    right[:, :half] = right[:, :half] + (ta[zl].astype(F32) + r3a[...].astype(F32)) * (1.0 / D)
    right_copy = pltpu.make_async_copy(right, right_hbm, load_sem.at[4])
    right_copy.start()

    wait_for(r2a, rsend_sem.at[3])
    wait_for(r3b, rsend_sem.at[4])
    wait_for(gain.at[0], send_sem.at[1])
    wait_for(wv.at[0], send_sem.at[2])
    wait_for(wo.at[0], send_sem.at[3])
    wait_for(rs, send_sem.at[4])
    wait_for(rs, send_sem.at[5])
    wait_for(sct, send_sem.at[6])
    wait_for(zs, send_sem.at[7])
    wait_for(wgt.at[other], send_sem.at[9])
    wait_for(sct, send_sem.at[10])
    wait_for(sct, out_sem.at[0])
    wait_for(sct, out_sem.at[1])

    @pl.when(s == 0)
    def _():
        wait_for(sct, send_sem.at[0])

    @pl.when(s < LATE - 1)
    def _():
        wait_for(outbuf, send_sem.at[8])

    @pl.when((s >= LATE - 2) & (s < 6))
    def _():
        wait_for(outbuf, send_sem.at[14])

    @pl.when((s >= LATE - 1) & (s < 7))
    def _():
        wait_for(wo.at[0], send_sem.at[11])
        wait_for(vin.at[:, 0], send_sem.at[13])

    @pl.when(s >= LATE)
    def _():
        wait_for(wop.at[0], send_sem.at[12])

    @pl.when((s >= LATE) & (s < 7) & jnp.logical_not(odd))
    def _():
        wait_for(vin.at[:, pl.ds(0, Y - 1)], send_sem.at[15])
        wait_for(vin.at[:, pl.ds(0, Y - 1)], send_sem.at[15])

    left_copy.wait()
    right_copy.wait()


def on_device(inputs, cotangent, norm_gain, value_weight, output_weight, left_old, right_old):
    any_space = pl.BlockSpec(memory_space=pl.ANY)
    dma = pltpu.SemaphoreType.DMA
    out, left, right = pl.pallas_call(
        kernel,
        out_shape=(
            jax.ShapeDtypeStruct((2, NC, T, W), BF16),
            jax.ShapeDtypeStruct((W, W), F32),
            jax.ShapeDtypeStruct((64, KV), F32),
        ),
        in_specs=[any_space] * 7,
        out_specs=(any_space, any_space, any_space),
        scratch_shapes=[
            pltpu.VMEM((2, W, KV), BF16),
            pltpu.VMEM((2, KV, W), BF16),
            pltpu.VMEM((2, KV, W), BF16),
            pltpu.VMEM((2, 1, W), BF16),
            pltpu.VMEM((NC, T, KV), BF16),
            pltpu.VMEM((NC, 2, T, W), BF16),
            pltpu.VMEM((NC, Y, OWN, KV), BF16),
            pltpu.VMEM((ROWS, W), BF16),
            pltpu.VMEM((NC, T, W), BF16),
            pltpu.VMEM((NC, 2, T, W), BF16),
            pltpu.VMEM((NC, Y, OWN, EXT), BF16),
            pltpu.VMEM((NC, Y - 1, OWN, EXT), BF16),
            pltpu.VMEM((NC, OWN, EXT), BF16),
            pltpu.VMEM((NC, OWN, EXT), BF16),
            pltpu.VMEM((NC, Y, OWN, EXT), BF16),
            pltpu.VMEM((ROWS, KV), BF16),
            pltpu.VMEM((W, KV), BF16),
            pltpu.VMEM((W, W), F32),
            pltpu.VMEM((64, KV), F32),
            pltpu.VMEM((2, Y, 2, 64, KV // 2), BF16),
            pltpu.VMEM((2, 2, Y, 64, KV // 2), BF16),
            pltpu.VMEM((Y, 2, 64, KV // 2), BF16),
            pltpu.VMEM((2, Y, 64, KV // 2), BF16),
            pltpu.VMEM((Y - 1, 2, 64, KV // 2), BF16),
            pltpu.VMEM((Y, 64, KV // 2), BF16),
            pltpu.VMEM((2, 64, KV // 2), BF16),
            pltpu.VMEM((Y, 64, KV // 2), BF16),
            pltpu.VMEM((64, KV // 2), BF16),
            pltpu.VMEM((Y - 1, 64, KV // 2), BF16),
            dma((6,)),
            dma((NC,)),
            dma((NC,)),
            dma((NC,)),
            dma((NC,)),
            dma((2,)),
            dma((2,)),
            dma((NC,)),
            dma((NC,)),
            dma((PIECES + 1,)),
            dma((16,)),
            dma((6,)),
            dma((6,)),
        ],
        compiler_params=pltpu.CompilerParams(
            collective_id=0, has_side_effects=True, vmem_limit_bytes=60 * 1024 * 1024
        ),
    )(
        inputs.reshape(2, NC, T, W),
        cotangent.reshape(2, NC, T, KV),
        norm_gain,
        value_weight[0],
        output_weight[0],
        left_old[0, 0],
        right_old[0],
    )
    return out.reshape(1, 8, 128, W), left[None, None], right[None]


def solution(mesh):
    placed = (
        P(None, None, "dp"),
        P("section", None, None, None),
        P("section", "dp"),
        P("section", "dp", None),
        P("section", None, "dp"),
        P("section", "dp", None, None),
        P("section", "dp", None),
    )
    return jax.shard_map(
        on_device,
        mesh=mesh,
        in_specs=placed,
        out_specs=(
            P("section", None, None, "dp"),
            P("section", "dp", None, None),
            P("section", "dp", None),
        ),
        check_vma=False,
    )
```

```python
import jax
import jax.numpy as jnp
from jax import lax
from jax.experimental import pallas as pl
from jax.experimental.pallas import tpu as pltpu
from jax.sharding import PartitionSpec as P

MESH = pl.DeviceIdType.MESH
F32 = jnp.float32
BF16 = jnp.bfloat16

D = 16384
W = 1024
KV = 1024
ROWS = 1024
T = 32
NC = ROWS // 2 // T
Y = 4
OWN = T // Y
EXT = KV + 128
LAG2, LAG3, LAG4 = 1, 2, 3
LAGP = 4
LATE = 4
PIECES = 4


def with_pair(rows, scalar):
    high = scalar.astype(BF16).astype(F32)
    low = scalar - high
    lane = lax.broadcasted_iota(jnp.int32, (rows.shape[0], 128), 1)
    pair = jnp.where(lane < 64, high, low)
    return jnp.concatenate([rows, pair], axis=1)


def pair_of(ext):
    return ext[:, KV : KV + 1] + ext[:, KV + 64 : KV + 65]


def kernel(
    x_hbm, cot_hbm, gain_ref, wv_hbm, wo_hbm, left_old_hbm, right_old_hbm,
    out_hbm, left_hbm, right_hbm,
    wv, wo, wop, gain, cot, xbuf, vin, sc, sct, outbuf, part, rs, zs, zr, val, wgt, gb, left, right,
    rpa, rpb, r1a, r1b, r2a, r2b, ta, tb, r3a, r3b,
    load_sem, x_sem, rs_sem, z_sem, ag_sem, out_sem, give_sem, v_sem, pre_sem, send_sem, r_sem, rsend_sem,
):
    s = lax.axis_index("section")
    d = lax.axis_index("dp")
    zl = d // 8
    core = lax.rem(d, 2)
    y = lax.rem(d, 8) // 2
    odd = lax.rem(s, 2) == 1
    zpeer = (s, lax.rem(d + 8, 16))
    cpeer = (s, d + 1 - 2 * core)

    def y_peer(offset):
        return (s, zl * 8 + lax.rem(y + offset, Y) * 2 + core)

    def rows_of(c):
        return pl.ds(pl.multiple_of(core * (ROWS // 2) + c * T, T), T)

    def remote(src, dst, send, recv, device):
        return pltpu.make_async_remote_copy(
            src_ref=src, dst_ref=dst, send_sem=send, recv_sem=recv, device_id=device, device_id_type=MESH
        )

    def wait_for(ref, sem):
        pltpu.make_async_copy(ref, ref, sem).wait()

    @pl.when(s == 0)
    def _():
        def body(c, carry):
            pltpu.make_async_copy(x_hbm.at[core, c], xbuf.at[c, core], x_sem.at[c]).start()
            return carry

        lax.fori_loop(0, NC, body, 0)

    pltpu.make_async_copy(wv_hbm, wv.at[core], load_sem.at[0]).start()
    pltpu.make_async_copy(wo_hbm, wo.at[core], load_sem.at[1]).start()
    load_cot = pltpu.make_async_copy(cot_hbm.at[core], cot, load_sem.at[2])
    load_left = pltpu.make_async_copy(left_old_hbm, left, load_sem.at[3])
    load_right = pltpu.make_async_copy(right_old_hbm, right, load_sem.at[4])
    pltpu.make_async_copy(gain_ref, gain.at[core], load_sem.at[5]).start()
    load_cot.start()
    load_left.start()
    load_right.start()

    barrier = pltpu.get_barrier_semaphore()
    for offset in range(1, Y):
        pl.semaphore_signal(barrier, inc=1, device_id=y_peer(offset), device_id_type=MESH)
    for step in (1, 7):
        for offset in range(Y):
            peer = (lax.rem(s + step, 8), y_peer(offset)[1])
            pl.semaphore_signal(barrier, inc=1, device_id=peer, device_id_type=MESH)
    for peer in (zpeer, cpeer, (lax.rem(s + 2, 8), d), (lax.rem(s + 6, 8), d)):
        pl.semaphore_signal(barrier, inc=1, device_id=peer, device_id_type=MESH)
    pl.semaphore_wait(barrier, Y - 1 + 2 * Y + 4)

    @pl.when(s == 0)
    def _():
        remote(x_hbm.at[1 - core, 0], xbuf.at[0, core], send_sem.at[0], x_sem.at[0], cpeer).start()

    remote(gain_ref, gain.at[core], send_sem.at[1], load_sem.at[5], cpeer).start()
    remote(wv_hbm, wv.at[core], send_sem.at[2], load_sem.at[0], cpeer).start()

    @pl.when(s == 0)
    def _():
        def body(c, carry):
            remote(x_hbm.at[1 - core, c], xbuf.at[c, core], send_sem.at[0], x_sem.at[c], cpeer).start()
            return carry

        lax.fori_loop(1, NC, body, 0)

    remote(wo_hbm, wo.at[core], send_sem.at[3], load_sem.at[1], cpeer).start()

    def piece(i):
        return pl.ds(i * (KV // PIECES), KV // PIECES)

    @pl.when((s >= LATE - 1) & (s < 7))
    def _():
        for i in range(PIECES):
            remote(
                wo_hbm.at[piece(i)], wop.at[core, piece(i)], send_sem.at[11], pre_sem.at[i], (s + 1, d)
            ).start()

    @pl.when(s >= LATE)
    def _():
        for i in range(PIECES):
            ours = wop.at[core, piece(i)]
            wait_for(ours, pre_sem.at[i])
            remote(ours, ours, send_sem.at[12], pre_sem.at[PIECES], cpeer).start()
        wait_for(wop.at[0], pre_sem.at[PIECES])

    wait_for(gain, load_sem.at[5])
    wait_for(wv, load_sem.at[0])

    def rs_copy(c, offset):
        return remote(
            part.at[c, lax.rem(y + offset, Y)], rs.at[c, offset - 1], send_sem.at[4], rs_sem.at[c], y_peer(offset)
        )

    def ag_copy(c, offset):
        return remote(val.at[c, y], val.at[c, y], send_sem.at[5], ag_sem.at[c], y_peer(offset))

    def stage1(c):
        wait_for(xbuf.at[c], x_sem.at[c])

        @pl.when(s >= LATE)
        def _():
            wait_for(vin.at[c], v_sem.at[c])
            before = vin[c].astype(F32).reshape(T, KV).astype(BF16)
            for h in range(2):
                made = xbuf[c, h].astype(F32) + jnp.dot(before, wop[h], preferred_element_type=F32)
                xbuf[c, h] = made.astype(BF16)

        product = None
        squares = None
        scaled = []
        for h in range(2):
            floats = xbuf[c, h].astype(F32)
            scaled.append((floats * gain[h].astype(F32)).astype(BF16))
            sums = jnp.sum(floats * floats, axis=1, keepdims=True)
            squares = sums if h == 0 else squares + sums
            dot = jnp.dot(scaled[h], wv[h], preferred_element_type=F32)
            product = dot if h == 0 else product + dot
        both = with_pair(product, squares)
        part[c] = both.reshape(Y, OWN, EXT).astype(BF16)
        for offset in range(1, Y):
            rs_copy(c, offset).start()

        @pl.when((s >= LATE) & (s < 7) & jnp.logical_not(odd))
        def _():
            remote(xbuf.at[c, 1], xbuf.at[c, 1], send_sem.at[15], x_sem.at[c], (s + 1, d)).start()

        sc[rows_of(c), :] = jnp.where(core == 0, scaled[0], scaled[1])
        sct[c] = jnp.where(core == 0, scaled[1], scaled[0])
        remote(sct.at[c], sc.at[rows_of(c)], send_sem.at[6], give_sem.at[0], cpeer).start()

    def stage2(c):
        wait_for(rs.at[c], rs_sem.at[c])
        total = part[c, y].astype(F32)
        for j in range(Y - 1):
            total += rs[c, j].astype(F32)
        zs[c] = with_pair(total[:, :KV], pair_of(total)).astype(BF16)
        remote(zs.at[c], zr.at[c], send_sem.at[7], z_sem.at[c], zpeer).start()

    def stage3(c):
        wait_for(zr.at[c], z_sem.at[c])
        total = zs[c].astype(F32) + zr[c].astype(F32)
        inv = lax.rsqrt(pair_of(total) / D + 0.25)
        val[c, y] = with_pair(inv * total[:, :KV], inv).astype(BF16)

        @pl.when((s >= LATE - 1) & (s < 7))
        def _():
            for offset in range(Y):
                remote(
                    val.at[c, y, :, pl.ds(0, KV)], vin.at[c, y], send_sem.at[13], v_sem.at[c], (s + 1, y_peer(offset)[1])
                ).start()

        for offset in range(1, Y):
            ag_copy(c, offset).start()

    def stage4(c):
        wait_for(rs.at[c], ag_sem.at[c])
        both = val[c].astype(F32).reshape(T, EXT)
        values = both[:, :KV].astype(BF16)
        for h in range(2):
            result = xbuf[c, h].astype(F32) + jnp.dot(values, wo[h], preferred_element_type=F32)
            outbuf[c, h] = result.astype(BF16)

        @pl.when(s < LATE - 1)
        def _():
            remote(outbuf.at[c], xbuf.at[c], send_sem.at[8], x_sem.at[c], (s + 1, d)).start()

        @pl.when((s >= LATE - 2) & (s < 6) & jnp.logical_not(odd))
        def _():
            remote(outbuf.at[c], xbuf.at[c], send_sem.at[14], x_sem.at[c], (s + 2, d)).start()

        @pl.when((s >= LATE - 2) & (s < 6) & odd)
        def _():
            remote(outbuf.at[c, 0], xbuf.at[c, 0], send_sem.at[14], x_sem.at[c], (s + 2, d)).start()

        wgt[rows_of(c), :] = (pair_of(both) * cot[c].astype(F32)).astype(BF16)
        remote(wgt.at[rows_of(c)], wgt.at[rows_of(c)], send_sem.at[9], give_sem.at[1], cpeer).start()
        pltpu.make_async_copy(outbuf.at[c, core], out_hbm.at[core, c], out_sem.at[0]).start()
        remote(outbuf.at[c, 1 - core], out_hbm.at[core, c], send_sem.at[10], out_sem.at[1], cpeer).start()

    def tick(k, carry):
        @pl.when(k == LAG4)
        def _():
            wait_for(wo, load_sem.at[1])
            load_cot.wait()

        def run(stage, lag, where=None):
            now = (k >= lag) & (k < NC + lag)

            @pl.when(now if where is None else now & where)
            def _():
                stage(k - lag)

        for stage, lag in ((stage1, 0),):
            run(stage, lag)
        run(stage4, LAGP, s >= LATE - 1)
        run(stage2, LAG2)
        run(stage3, LAG3)
        run(stage4, LAG4, s < LATE - 1)
        return carry

    lax.fori_loop(0, NC + LAGP, tick, 0)

    over_rows = (((0,), (0,)), ((), ()))
    over_cols = (((1,), (1,)), ((), ()))
    STEP = 256

    def block(i):
        return pl.ds(pl.multiple_of(i * STEP, STEP), STEP)

    other = pl.ds(pl.multiple_of((1 - core) * (ROWS // 2), ROWS // 2), ROWS // 2)
    wait_for(sc.at[other], give_sem.at[0])
    wait_for(wgt.at[other], give_sem.at[1])

    def grad_block(i, carry):
        gb[block(i), :] = lax.dot_general(
            sc[:, block(i)], wgt[...], over_rows, preferred_element_type=F32
        ).astype(BF16)
        return carry

    lax.fori_loop(0, W // STEP, grad_block, 0)

    half = KV // 2

    def right_rows(i, h):
        return lax.dot_general(
            gb[:, block(i)], gb[:, h * half : (h + 1) * half], over_rows, preferred_element_type=F32
        ).astype(BF16)

    def right_b(i, carry):
        rows = right_rows(i, 1)
        for j in range(4):
            rpb[j % 2, i // 2, 2 * lax.rem(i, 2) + j // 2] = rows[64 * j : 64 * (j + 1), :]
        return carry

    def right_a(i, carry):
        rows = right_rows(i, 0)
        for j in range(4):
            rpa[j % 2, 2 * lax.rem(i, 2) + j // 2, i // 2] = rows[64 * j : 64 * (j + 1), :]
        return carry

    core_b = remote(rpb.at[1 - core], r1b, rsend_sem.at[0], r_sem.at[0], cpeer)
    core_a = remote(rpa.at[1 - core], r1a, rsend_sem.at[1], r_sem.at[1], cpeer)
    lax.fori_loop(0, KV // STEP, right_b, 0)
    core_b.start()
    lax.fori_loop(0, KV // STEP, right_a, 0)
    core_a.start()

    def left_block(i, carry):
        add = lax.dot_general(gb[block(i), :], gb[...], over_cols, preferred_element_type=F32)
        left[block(i), :] = left[block(i), :] + add * (1.0 / 1024)
        return carry

    core_b.wait()
    r1b[...] = (rpb[core].astype(F32) + r1b[...].astype(F32)).astype(BF16)
    z_b = remote(r1b.at[1 - zl], r2b, rsend_sem.at[2], r_sem.at[2], zpeer)
    z_b.start()
    core_a.wait()
    r1a[...] = (rpa[core].astype(F32) + r1a[...].astype(F32)).astype(BF16)
    for offset in range(1, Y):
        remote(
            r1a.at[lax.rem(y + offset, Y)], r2a.at[offset - 1], rsend_sem.at[3], r_sem.at[3], y_peer(offset)
        ).start()
    load_left.wait()
    load_right.wait()
    lax.fori_loop(0, W // STEP, left_block, 0)
    left_copy = pltpu.make_async_copy(left, left_hbm, load_sem.at[3])
    left_copy.start()
    z_b.wait()
    tb[...] = (r1b[zl].astype(F32) + r2b[...].astype(F32)).astype(BF16)
    for offset in range(1, Y):
        remote(
            tb.at[lax.rem(y + offset, Y)], r3b.at[offset - 1], rsend_sem.at[4], r_sem.at[4], y_peer(offset)
        ).start()
    wait_for(r2a, r_sem.at[3])
    summed = r1a[y].astype(F32)
    for j in range(Y - 1):
        summed += r2a[j].astype(F32)
    ta[...] = summed.astype(BF16)
    z_a = remote(ta.at[1 - zl], r3a, rsend_sem.at[5], r_sem.at[5], zpeer)
    z_a.start()
    wait_for(r3b, r_sem.at[4])
    summed = tb[y].astype(F32)
    for j in range(Y - 1):
        summed += r3b[j].astype(F32)
    right[:, half:] = right[:, half:] + summed * (1.0 / D)
    z_a.wait()
    right[:, :half] = right[:, :half] + (ta[zl].astype(F32) + r3a[...].astype(F32)) * (1.0 / D)
    right_copy = pltpu.make_async_copy(right, right_hbm, load_sem.at[4])
    right_copy.start()

    wait_for(r2a, rsend_sem.at[3])
    wait_for(r3b, rsend_sem.at[4])
    wait_for(gain.at[0], send_sem.at[1])
    wait_for(wv.at[0], send_sem.at[2])
    wait_for(wo.at[0], send_sem.at[3])
    wait_for(rs, send_sem.at[4])
    wait_for(rs, send_sem.at[5])
    wait_for(sct, send_sem.at[6])
    wait_for(zs, send_sem.at[7])
    wait_for(wgt.at[other], send_sem.at[9])
    wait_for(sct, send_sem.at[10])
    wait_for(sct, out_sem.at[0])
    wait_for(sct, out_sem.at[1])

    @pl.when(s == 0)
    def _():
        wait_for(sct, send_sem.at[0])

    @pl.when(s < LATE - 1)
    def _():
        wait_for(outbuf, send_sem.at[8])

    @pl.when((s >= LATE - 2) & (s < 6) & jnp.logical_not(odd))
    def _():
        wait_for(outbuf, send_sem.at[14])

    @pl.when((s >= LATE - 2) & (s < 6) & odd)
    def _():
        wait_for(sct, send_sem.at[14])

    @pl.when((s >= LATE - 1) & (s < 7))
    def _():
        wait_for(wo.at[0], send_sem.at[11])
        wait_for(vin, send_sem.at[13])

    @pl.when(s >= LATE)
    def _():
        wait_for(wop.at[0], send_sem.at[12])

    @pl.when((s >= LATE) & (s < 7) & jnp.logical_not(odd))
    def _():
        wait_for(sct, send_sem.at[15])

    left_copy.wait()
    right_copy.wait()


def on_device(inputs, cotangent, norm_gain, value_weight, output_weight, left_old, right_old):
    any_space = pl.BlockSpec(memory_space=pl.ANY)
    dma = pltpu.SemaphoreType.DMA
    out, left, right = pl.pallas_call(
        kernel,
        out_shape=(
            jax.ShapeDtypeStruct((2, NC, T, W), BF16),
            jax.ShapeDtypeStruct((W, W), F32),
            jax.ShapeDtypeStruct((64, KV), F32),
        ),
        in_specs=[any_space] * 7,
        out_specs=(any_space, any_space, any_space),
        scratch_shapes=[
            pltpu.VMEM((2, W, KV), BF16),
            pltpu.VMEM((2, KV, W), BF16),
            pltpu.VMEM((2, KV, W), BF16),
            pltpu.VMEM((2, 1, W), BF16),
            pltpu.VMEM((NC, T, KV), BF16),
            pltpu.VMEM((NC, 2, T, W), BF16),
            pltpu.VMEM((NC, Y, OWN, KV), BF16),
            pltpu.VMEM((ROWS, W), BF16),
            pltpu.VMEM((NC, T, W), BF16),
            pltpu.VMEM((NC, 2, T, W), BF16),
            pltpu.VMEM((NC, Y, OWN, EXT), BF16),
            pltpu.VMEM((NC, Y - 1, OWN, EXT), BF16),
            pltpu.VMEM((NC, OWN, EXT), BF16),
            pltpu.VMEM((NC, OWN, EXT), BF16),
            pltpu.VMEM((NC, Y, OWN, EXT), BF16),
            pltpu.VMEM((ROWS, KV), BF16),
            pltpu.VMEM((W, KV), BF16),
            pltpu.VMEM((W, W), F32),
            pltpu.VMEM((64, KV), F32),
            pltpu.VMEM((2, Y, 2, 64, KV // 2), BF16),
            pltpu.VMEM((2, 2, Y, 64, KV // 2), BF16),
            pltpu.VMEM((Y, 2, 64, KV // 2), BF16),
            pltpu.VMEM((2, Y, 64, KV // 2), BF16),
            pltpu.VMEM((Y - 1, 2, 64, KV // 2), BF16),
            pltpu.VMEM((Y, 64, KV // 2), BF16),
            pltpu.VMEM((2, 64, KV // 2), BF16),
            pltpu.VMEM((Y, 64, KV // 2), BF16),
            pltpu.VMEM((64, KV // 2), BF16),
            pltpu.VMEM((Y - 1, 64, KV // 2), BF16),
            dma((6,)),
            dma((NC,)),
            dma((NC,)),
            dma((NC,)),
            dma((NC,)),
            dma((2,)),
            dma((2,)),
            dma((NC,)),
            dma((PIECES + 1,)),
            dma((16,)),
            dma((6,)),
            dma((6,)),
        ],
        compiler_params=pltpu.CompilerParams(
            collective_id=0, has_side_effects=True, vmem_limit_bytes=60 * 1024 * 1024
        ),
    )(
        inputs.reshape(2, NC, T, W),
        cotangent.reshape(2, NC, T, KV),
        norm_gain,
        value_weight[0],
        output_weight[0],
        left_old[0, 0],
        right_old[0],
    )
    return out.reshape(1, 8, 128, W), left[None, None], right[None]


def solution(mesh):
    placed = (
        P(None, None, "dp"),
        P("section", None, None, None),
        P("section", "dp"),
        P("section", "dp", None),
        P("section", None, "dp"),
        P("section", "dp", None, None),
        P("section", "dp", None),
    )
    return jax.shard_map(
        on_device,
        mesh=mesh,
        in_specs=placed,
        out_specs=(
            P("section", None, None, "dp"),
            P("section", "dp", None, None),
            P("section", "dp", None),
        ),
        check_vma=False,
    )
```

```python
import jax
import jax.numpy as jnp
from jax import lax
from jax.experimental import pallas as pl
from jax.experimental.pallas import tpu as pltpu
from jax.sharding import PartitionSpec as P

MESH = pl.DeviceIdType.MESH
F32 = jnp.float32
BF16 = jnp.bfloat16

D = 16384
W = 1024
KV = 1024
ROWS = 1024
T = 32
NC = ROWS // 2 // T
Y = 4
OWN = T // Y
EXT = KV + 128
LAG2, LAG3, LAG4 = 1, 2, 3
LAGP = 5
LATE = 4
PIECES = 4


def with_pair(rows, scalar):
    high = scalar.astype(BF16).astype(F32)
    low = scalar - high
    lane = lax.broadcasted_iota(jnp.int32, (rows.shape[0], 128), 1)
    pair = jnp.where(lane < 64, high, low)
    return jnp.concatenate([rows, pair], axis=1)


def pair_of(ext):
    return ext[:, KV : KV + 1] + ext[:, KV + 64 : KV + 65]


def kernel(
    x_hbm, cot_hbm, gain_ref, wv_hbm, wo_hbm, left_old_hbm, right_old_hbm,
    out_hbm, left_hbm, right_hbm,
    wv, wo, wop, gain, cot, xbuf, vin, sc, sct, outbuf, part, rs, zs, zr, val, wgt, gb, left, right,
    rpa, rpb, r1a, r1b, r2a, r2b, ta, tb, r3a, r3b,
    load_sem, x_sem, rs_sem, z_sem, ag_sem, out_sem, give_sem, v_sem, pre_sem, send_sem, r_sem, rsend_sem,
):
    s = lax.axis_index("section")
    d = lax.axis_index("dp")
    zl = d // 8
    core = lax.rem(d, 2)
    y = lax.rem(d, 8) // 2
    odd = lax.rem(s, 2) == 1
    zpeer = (s, lax.rem(d + 8, 16))
    cpeer = (s, d + 1 - 2 * core)

    def y_peer(offset):
        return (s, zl * 8 + lax.rem(y + offset, Y) * 2 + core)

    def rows_of(c):
        return pl.ds(pl.multiple_of(core * (ROWS // 2) + c * T, T), T)

    def remote(src, dst, send, recv, device):
        return pltpu.make_async_remote_copy(
            src_ref=src, dst_ref=dst, send_sem=send, recv_sem=recv, device_id=device, device_id_type=MESH
        )

    def wait_for(ref, sem):
        pltpu.make_async_copy(ref, ref, sem).wait()

    @pl.when(s == 0)
    def _():
        def body(c, carry):
            pltpu.make_async_copy(x_hbm.at[core, c], xbuf.at[c, core], x_sem.at[c]).start()
            return carry

        lax.fori_loop(0, NC, body, 0)

    pltpu.make_async_copy(wv_hbm, wv.at[core], load_sem.at[0]).start()
    pltpu.make_async_copy(wo_hbm, wo.at[core], load_sem.at[1]).start()
    load_cot = pltpu.make_async_copy(cot_hbm.at[core], cot, load_sem.at[2])
    load_left = pltpu.make_async_copy(left_old_hbm, left, load_sem.at[3])
    load_right = pltpu.make_async_copy(right_old_hbm, right, load_sem.at[4])
    pltpu.make_async_copy(gain_ref, gain.at[core], load_sem.at[5]).start()
    load_cot.start()
    load_left.start()
    load_right.start()

    barrier = pltpu.get_barrier_semaphore()
    for offset in range(1, Y):
        pl.semaphore_signal(barrier, inc=1, device_id=y_peer(offset), device_id_type=MESH)
    for step in (1, 7):
        for offset in range(Y):
            peer = (lax.rem(s + step, 8), y_peer(offset)[1])
            pl.semaphore_signal(barrier, inc=1, device_id=peer, device_id_type=MESH)
    for peer in (zpeer, cpeer, (lax.rem(s + 2, 8), d), (lax.rem(s + 6, 8), d)):
        pl.semaphore_signal(barrier, inc=1, device_id=peer, device_id_type=MESH)
    pl.semaphore_wait(barrier, Y - 1 + 2 * Y + 4)

    @pl.when(s == 0)
    def _():
        remote(x_hbm.at[1 - core, 0], xbuf.at[0, core], send_sem.at[0], x_sem.at[0], cpeer).start()

    remote(gain_ref, gain.at[core], send_sem.at[1], load_sem.at[5], cpeer).start()
    remote(wv_hbm, wv.at[core], send_sem.at[2], load_sem.at[0], cpeer).start()

    @pl.when(s == 0)
    def _():
        def body(c, carry):
            remote(x_hbm.at[1 - core, c], xbuf.at[c, core], send_sem.at[0], x_sem.at[c], cpeer).start()
            return carry

        lax.fori_loop(1, NC, body, 0)

    remote(wo_hbm, wo.at[core], send_sem.at[3], load_sem.at[1], cpeer).start()

    def piece(i):
        return pl.ds(i * (KV // PIECES), KV // PIECES)

    @pl.when((s >= LATE - 1) & (s < 7))
    def _():
        for i in range(PIECES):
            remote(
                wo_hbm.at[piece(i)], wop.at[core, piece(i)], send_sem.at[11], pre_sem.at[i], (s + 1, d)
            ).start()

    @pl.when(s >= LATE)
    def _():
        for i in range(PIECES):
            ours = wop.at[core, piece(i)]
            wait_for(ours, pre_sem.at[i])
            remote(ours, ours, send_sem.at[12], pre_sem.at[PIECES], cpeer).start()
        wait_for(wop.at[0], pre_sem.at[PIECES])

    wait_for(gain, load_sem.at[5])
    wait_for(wv, load_sem.at[0])

    def rs_copy(c, offset):
        return remote(
            part.at[c, lax.rem(y + offset, Y)], rs.at[c, offset - 1], send_sem.at[4], rs_sem.at[c], y_peer(offset)
        )

    def ag_copy(c, offset):
        return remote(val.at[c, y], val.at[c, y], send_sem.at[5], ag_sem.at[c], y_peer(offset))

    def stage1(c):
        wait_for(xbuf.at[c], x_sem.at[c])

        @pl.when(s >= LATE)
        def _():
            wait_for(vin.at[c], v_sem.at[c])
            before = vin[c].astype(F32).reshape(T, KV).astype(BF16)
            for h in range(2):
                made = xbuf[c, h].astype(F32) + jnp.dot(before, wop[h], preferred_element_type=F32)
                xbuf[c, h] = made.astype(BF16)

        product = None
        squares = None
        scaled = []
        for h in range(2):
            floats = xbuf[c, h].astype(F32)
            scaled.append((floats * gain[h].astype(F32)).astype(BF16))
            sums = jnp.sum(floats * floats, axis=1, keepdims=True)
            squares = sums if h == 0 else squares + sums
            dot = jnp.dot(scaled[h], wv[h], preferred_element_type=F32)
            product = dot if h == 0 else product + dot
        both = with_pair(product, squares)
        part[c] = both.reshape(Y, OWN, EXT).astype(BF16)
        for offset in range(1, Y):
            rs_copy(c, offset).start()

        @pl.when((s >= LATE) & (s < 7) & jnp.logical_not(odd))
        def _():
            remote(xbuf.at[c, 1], xbuf.at[c, 1], send_sem.at[15], x_sem.at[c], (s + 1, d)).start()

        sc[rows_of(c), :] = jnp.where(core == 0, scaled[0], scaled[1])
        sct[c] = jnp.where(core == 0, scaled[1], scaled[0])
        remote(sct.at[c], sc.at[rows_of(c)], send_sem.at[6], give_sem.at[0], cpeer).start()

    def stage2(c):
        wait_for(rs.at[c], rs_sem.at[c])
        total = part[c, y].astype(F32)
        for j in range(Y - 1):
            total += rs[c, j].astype(F32)
        zs[c] = with_pair(total[:, :KV], pair_of(total)).astype(BF16)
        remote(zs.at[c], zr.at[c], send_sem.at[7], z_sem.at[c], zpeer).start()

    def stage3(c):
        wait_for(zr.at[c], z_sem.at[c])
        total = zs[c].astype(F32) + zr[c].astype(F32)
        inv = lax.rsqrt(pair_of(total) / D + 0.25)
        val[c, y] = with_pair(inv * total[:, :KV], inv).astype(BF16)

        @pl.when((s >= LATE - 1) & (s < 7))
        def _():
            for offset in range(Y):
                remote(
                    val.at[c, y, :, pl.ds(0, KV)], vin.at[c, y], send_sem.at[13], v_sem.at[c], (s + 1, y_peer(offset)[1])
                ).start()

        for offset in range(1, Y):
            ag_copy(c, offset).start()

    def stage4(c):
        wait_for(rs.at[c], ag_sem.at[c])
        both = val[c].astype(F32).reshape(T, EXT)
        values = both[:, :KV].astype(BF16)
        for h in range(2):
            result = xbuf[c, h].astype(F32) + jnp.dot(values, wo[h], preferred_element_type=F32)
            outbuf[c, h] = result.astype(BF16)

        @pl.when(s < LATE - 1)
        def _():
            remote(outbuf.at[c], xbuf.at[c], send_sem.at[8], x_sem.at[c], (s + 1, d)).start()

        @pl.when((s >= LATE - 2) & (s < 6) & jnp.logical_not(odd))
        def _():
            remote(outbuf.at[c], xbuf.at[c], send_sem.at[14], x_sem.at[c], (s + 2, d)).start()

        @pl.when((s >= LATE - 2) & (s < 6) & odd)
        def _():
            remote(outbuf.at[c, 0], xbuf.at[c, 0], send_sem.at[14], x_sem.at[c], (s + 2, d)).start()

        wgt[rows_of(c), :] = (pair_of(both) * cot[c].astype(F32)).astype(BF16)
        remote(wgt.at[rows_of(c)], wgt.at[rows_of(c)], send_sem.at[9], give_sem.at[1], cpeer).start()
        pltpu.make_async_copy(outbuf.at[c, core], out_hbm.at[core, c], out_sem.at[0]).start()
        remote(outbuf.at[c, 1 - core], out_hbm.at[core, c], send_sem.at[10], out_sem.at[1], cpeer).start()

    def tick(k, carry):
        @pl.when(k == LAG4)
        def _():
            wait_for(wo, load_sem.at[1])
            load_cot.wait()

        def run(stage, lag, where=None):
            now = (k >= lag) & (k < NC + lag)

            @pl.when(now if where is None else now & where)
            def _():
                stage(k - lag)

        for stage, lag in ((stage1, 0),):
            run(stage, lag)
        run(stage4, LAGP, s >= LATE - 1)
        run(stage2, LAG2)
        run(stage3, LAG3)
        run(stage4, LAG4, s < LATE - 1)
        return carry

    lax.fori_loop(0, NC + LAGP, tick, 0)

    over_rows = (((0,), (0,)), ((), ()))
    over_cols = (((1,), (1,)), ((), ()))
    STEP = 256

    def block(i):
        return pl.ds(pl.multiple_of(i * STEP, STEP), STEP)

    other = pl.ds(pl.multiple_of((1 - core) * (ROWS // 2), ROWS // 2), ROWS // 2)
    wait_for(sc.at[other], give_sem.at[0])
    wait_for(wgt.at[other], give_sem.at[1])

    def grad_block(i, carry):
        gb[block(i), :] = lax.dot_general(
            sc[:, block(i)], wgt[...], over_rows, preferred_element_type=F32
        ).astype(BF16)
        return carry

    lax.fori_loop(0, W // STEP, grad_block, 0)

    half = KV // 2

    def right_rows(i, h):
        return lax.dot_general(
            gb[:, block(i)], gb[:, h * half : (h + 1) * half], over_rows, preferred_element_type=F32
        ).astype(BF16)

    def right_b(i, carry):
        rows = right_rows(i, 1)
        for j in range(4):
            rpb[j % 2, i // 2, 2 * lax.rem(i, 2) + j // 2] = rows[64 * j : 64 * (j + 1), :]
        return carry

    def right_a(i, carry):
        rows = right_rows(i, 0)
        for j in range(4):
            rpa[j % 2, 2 * lax.rem(i, 2) + j // 2, i // 2] = rows[64 * j : 64 * (j + 1), :]
        return carry

    core_b = remote(rpb.at[1 - core], r1b, rsend_sem.at[0], r_sem.at[0], cpeer)
    core_a = remote(rpa.at[1 - core], r1a, rsend_sem.at[1], r_sem.at[1], cpeer)
    lax.fori_loop(0, KV // STEP, right_b, 0)
    core_b.start()
    lax.fori_loop(0, KV // STEP, right_a, 0)
    core_a.start()

    def left_block(i, carry):
        add = lax.dot_general(gb[block(i), :], gb[...], over_cols, preferred_element_type=F32)
        left[block(i), :] = left[block(i), :] + add * (1.0 / 1024)
        return carry

    core_b.wait()
    r1b[...] = (rpb[core].astype(F32) + r1b[...].astype(F32)).astype(BF16)
    z_b = remote(r1b.at[1 - zl], r2b, rsend_sem.at[2], r_sem.at[2], zpeer)
    z_b.start()
    core_a.wait()
    r1a[...] = (rpa[core].astype(F32) + r1a[...].astype(F32)).astype(BF16)
    for offset in range(1, Y):
        remote(
            r1a.at[lax.rem(y + offset, Y)], r2a.at[offset - 1], rsend_sem.at[3], r_sem.at[3], y_peer(offset)
        ).start()
    load_left.wait()
    load_right.wait()
    lax.fori_loop(0, W // STEP, left_block, 0)
    left_copy = pltpu.make_async_copy(left, left_hbm, load_sem.at[3])
    left_copy.start()
    z_b.wait()
    tb[...] = (r1b[zl].astype(F32) + r2b[...].astype(F32)).astype(BF16)
    for offset in range(1, Y):
        remote(
            tb.at[lax.rem(y + offset, Y)], r3b.at[offset - 1], rsend_sem.at[4], r_sem.at[4], y_peer(offset)
        ).start()
    wait_for(r2a, r_sem.at[3])
    summed = r1a[y].astype(F32)
    for j in range(Y - 1):
        summed += r2a[j].astype(F32)
    ta[...] = summed.astype(BF16)
    z_a = remote(ta.at[1 - zl], r3a, rsend_sem.at[5], r_sem.at[5], zpeer)
    z_a.start()
    wait_for(r3b, r_sem.at[4])
    summed = tb[y].astype(F32)
    for j in range(Y - 1):
        summed += r3b[j].astype(F32)
    right[:, half:] = right[:, half:] + summed * (1.0 / D)
    z_a.wait()
    right[:, :half] = right[:, :half] + (ta[zl].astype(F32) + r3a[...].astype(F32)) * (1.0 / D)
    right_copy = pltpu.make_async_copy(right, right_hbm, load_sem.at[4])
    right_copy.start()

    wait_for(r2a, rsend_sem.at[3])
    wait_for(r3b, rsend_sem.at[4])
    wait_for(gain.at[0], send_sem.at[1])
    wait_for(wv.at[0], send_sem.at[2])
    wait_for(wo.at[0], send_sem.at[3])
    wait_for(rs, send_sem.at[4])
    wait_for(rs, send_sem.at[5])
    wait_for(sct, send_sem.at[6])
    wait_for(zs, send_sem.at[7])
    wait_for(wgt.at[other], send_sem.at[9])
    wait_for(sct, send_sem.at[10])
    wait_for(sct, out_sem.at[0])
    wait_for(sct, out_sem.at[1])

    @pl.when(s == 0)
    def _():
        wait_for(sct, send_sem.at[0])

    @pl.when(s < LATE - 1)
    def _():
        wait_for(outbuf, send_sem.at[8])

    @pl.when((s >= LATE - 2) & (s < 6) & jnp.logical_not(odd))
    def _():
        wait_for(outbuf, send_sem.at[14])

    @pl.when((s >= LATE - 2) & (s < 6) & odd)
    def _():
        wait_for(sct, send_sem.at[14])

    @pl.when((s >= LATE - 1) & (s < 7))
    def _():
        wait_for(wo.at[0], send_sem.at[11])
        wait_for(vin, send_sem.at[13])

    @pl.when(s >= LATE)
    def _():
        wait_for(wop.at[0], send_sem.at[12])

    @pl.when((s >= LATE) & (s < 7) & jnp.logical_not(odd))
    def _():
        wait_for(sct, send_sem.at[15])

    left_copy.wait()
    right_copy.wait()


def on_device(inputs, cotangent, norm_gain, value_weight, output_weight, left_old, right_old):
    any_space = pl.BlockSpec(memory_space=pl.ANY)
    dma = pltpu.SemaphoreType.DMA
    out, left, right = pl.pallas_call(
        kernel,
        out_shape=(
            jax.ShapeDtypeStruct((2, NC, T, W), BF16),
            jax.ShapeDtypeStruct((W, W), F32),
            jax.ShapeDtypeStruct((64, KV), F32),
        ),
        in_specs=[any_space] * 7,
        out_specs=(any_space, any_space, any_space),
        scratch_shapes=[
            pltpu.VMEM((2, W, KV), BF16),
            pltpu.VMEM((2, KV, W), BF16),
            pltpu.VMEM((2, KV, W), BF16),
            pltpu.VMEM((2, 1, W), BF16),
            pltpu.VMEM((NC, T, KV), BF16),
            pltpu.VMEM((NC, 2, T, W), BF16),
            pltpu.VMEM((NC, Y, OWN, KV), BF16),
            pltpu.VMEM((ROWS, W), BF16),
            pltpu.VMEM((NC, T, W), BF16),
            pltpu.VMEM((NC, 2, T, W), BF16),
            pltpu.VMEM((NC, Y, OWN, EXT), BF16),
            pltpu.VMEM((NC, Y - 1, OWN, EXT), BF16),
            pltpu.VMEM((NC, OWN, EXT), BF16),
            pltpu.VMEM((NC, OWN, EXT), BF16),
            pltpu.VMEM((NC, Y, OWN, EXT), BF16),
            pltpu.VMEM((ROWS, KV), BF16),
            pltpu.VMEM((W, KV), BF16),
            pltpu.VMEM((W, W), F32),
            pltpu.VMEM((64, KV), F32),
            pltpu.VMEM((2, Y, 2, 64, KV // 2), BF16),
            pltpu.VMEM((2, 2, Y, 64, KV // 2), BF16),
            pltpu.VMEM((Y, 2, 64, KV // 2), BF16),
            pltpu.VMEM((2, Y, 64, KV // 2), BF16),
            pltpu.VMEM((Y - 1, 2, 64, KV // 2), BF16),
            pltpu.VMEM((Y, 64, KV // 2), BF16),
            pltpu.VMEM((2, 64, KV // 2), BF16),
            pltpu.VMEM((Y, 64, KV // 2), BF16),
            pltpu.VMEM((64, KV // 2), BF16),
            pltpu.VMEM((Y - 1, 64, KV // 2), BF16),
            dma((6,)),
            dma((NC,)),
            dma((NC,)),
            dma((NC,)),
            dma((NC,)),
            dma((2,)),
            dma((2,)),
            dma((NC,)),
            dma((PIECES + 1,)),
            dma((16,)),
            dma((6,)),
            dma((6,)),
        ],
        compiler_params=pltpu.CompilerParams(
            collective_id=0, has_side_effects=True, vmem_limit_bytes=60 * 1024 * 1024,
        ),
    )(
        inputs.reshape(2, NC, T, W),
        cotangent.reshape(2, NC, T, KV),
        norm_gain,
        value_weight[0],
        output_weight[0],
        left_old[0, 0],
        right_old[0],
    )
    return out.reshape(1, 8, 128, W), left[None, None], right[None]


def solution(mesh):
    placed = (
        P(None, None, "dp"),
        P("section", None, None, None),
        P("section", "dp"),
        P("section", "dp", None),
        P("section", None, "dp"),
        P("section", "dp", None, None),
        P("section", "dp", None),
    )
    return jax.shard_map(
        on_device,
        mesh=mesh,
        in_specs=placed,
        out_specs=(
            P("section", None, None, "dp"),
            P("section", "dp", None, None),
            P("section", "dp", None),
        ),
        check_vma=False,
    )
```

```python
import jax
import jax.numpy as jnp
from jax import lax
from jax.experimental import pallas as pl
from jax.experimental.pallas import tpu as pltpu
from jax.sharding import PartitionSpec as P

MESH = pl.DeviceIdType.MESH
F32 = jnp.float32
BF16 = jnp.bfloat16

D = 16384
W = 1024
KV = 1024
ROWS = 1024
T = 32
NC = ROWS // 2 // T
Y = 4
FAR_FIRST = (2, 1, 3)
OWN = T // Y
EXT = KV + 128
LAG2, LAG3, LAG4 = 1, 2, 3
LAGP = 5
LATE = 4
PIECES = 4


def with_pair(rows, scalar):
    high = scalar.astype(BF16).astype(F32)
    low = scalar - high
    lane = lax.broadcasted_iota(jnp.int32, (rows.shape[0], 128), 1)
    pair = jnp.where(lane < 64, high, low)
    return jnp.concatenate([rows, pair], axis=1)


def pair_of(ext):
    return ext[:, KV : KV + 1] + ext[:, KV + 64 : KV + 65]


def kernel(
    x_hbm, cot_hbm, gain_ref, wv_hbm, wo_hbm, left_old_hbm, right_old_hbm,
    out_hbm, left_hbm, right_hbm,
    wv, wo, wop, gain, cot, xbuf, vin, sc, sct, outbuf, part, rs, zs, zr, val, wgt, gb, left, right,
    rpa, rpb, r1a, r1b, r2a, r2b, ta, tb, r3a, r3b,
    load_sem, x_sem, rs_sem, z_sem, ag_sem, out_sem, give_sem, v_sem, pre_sem, send_sem, r_sem, rsend_sem,
):
    s = lax.axis_index("section")
    d = lax.axis_index("dp")
    zl = d // 8
    core = lax.rem(d, 2)
    y = lax.rem(d, 8) // 2
    odd = lax.rem(s, 2) == 1
    zpeer = (s, lax.rem(d + 8, 16))
    cpeer = (s, d + 1 - 2 * core)

    def y_peer(offset):
        return (s, zl * 8 + lax.rem(y + offset, Y) * 2 + core)

    def rows_of(c):
        return pl.ds(pl.multiple_of(core * (ROWS // 2) + c * T, T), T)

    def remote(src, dst, send, recv, device):
        return pltpu.make_async_remote_copy(
            src_ref=src, dst_ref=dst, send_sem=send, recv_sem=recv, device_id=device, device_id_type=MESH
        )

    def wait_for(ref, sem):
        pltpu.make_async_copy(ref, ref, sem).wait()

    @pl.when(s == 0)
    def _():
        def body(c, carry):
            pltpu.make_async_copy(x_hbm.at[core, c], xbuf.at[c, core], x_sem.at[c]).start()
            return carry

        lax.fori_loop(0, NC, body, 0)

    pltpu.make_async_copy(wv_hbm, wv.at[core], load_sem.at[0]).start()
    pltpu.make_async_copy(wo_hbm, wo.at[core], load_sem.at[1]).start()
    load_cot = pltpu.make_async_copy(cot_hbm.at[core], cot, load_sem.at[2])
    load_left = pltpu.make_async_copy(left_old_hbm, left, load_sem.at[3])
    load_right = pltpu.make_async_copy(right_old_hbm, right, load_sem.at[4])
    pltpu.make_async_copy(gain_ref, gain.at[core], load_sem.at[5]).start()
    load_cot.start()
    load_left.start()
    load_right.start()

    barrier = pltpu.get_barrier_semaphore()
    for offset in range(1, Y):
        pl.semaphore_signal(barrier, inc=1, device_id=y_peer(offset), device_id_type=MESH)
    for step in (1, 7):
        for offset in range(Y):
            peer = (lax.rem(s + step, 8), y_peer(offset)[1])
            pl.semaphore_signal(barrier, inc=1, device_id=peer, device_id_type=MESH)
    for peer in (zpeer, cpeer, (lax.rem(s + 2, 8), d), (lax.rem(s + 6, 8), d)):
        pl.semaphore_signal(barrier, inc=1, device_id=peer, device_id_type=MESH)
    pl.semaphore_wait(barrier, Y - 1 + 2 * Y + 4)

    @pl.when(s == 0)
    def _():
        remote(x_hbm.at[1 - core, 0], xbuf.at[0, core], send_sem.at[0], x_sem.at[0], cpeer).start()

    remote(gain_ref, gain.at[core], send_sem.at[1], load_sem.at[5], cpeer).start()
    remote(wv_hbm, wv.at[core], send_sem.at[2], load_sem.at[0], cpeer).start()

    @pl.when(s == 0)
    def _():
        def body(c, carry):
            remote(x_hbm.at[1 - core, c], xbuf.at[c, core], send_sem.at[0], x_sem.at[c], cpeer).start()
            return carry

        lax.fori_loop(1, NC, body, 0)

    remote(wo_hbm, wo.at[core], send_sem.at[3], load_sem.at[1], cpeer).start()

    def piece(i):
        return pl.ds(i * (KV // PIECES), KV // PIECES)

    @pl.when((s >= LATE - 1) & (s < 7))
    def _():
        for i in range(PIECES):
            remote(
                wo_hbm.at[piece(i)], wop.at[core, piece(i)], send_sem.at[11], pre_sem.at[i], (s + 1, d)
            ).start()

    @pl.when(s >= LATE)
    def _():
        for i in range(PIECES):
            ours = wop.at[core, piece(i)]
            wait_for(ours, pre_sem.at[i])
            remote(ours, ours, send_sem.at[12], pre_sem.at[PIECES], cpeer).start()
        wait_for(wop.at[0], pre_sem.at[PIECES])

    wait_for(gain, load_sem.at[5])
    wait_for(wv, load_sem.at[0])

    def rs_copy(c, offset):
        return remote(
            part.at[c, lax.rem(y + offset, Y)], rs.at[c, offset - 1], send_sem.at[4], rs_sem.at[c], y_peer(offset)
        )

    def ag_copy(c, offset):
        return remote(val.at[c, y], val.at[c, y], send_sem.at[5], ag_sem.at[c], y_peer(offset))

    def stage1(c):
        wait_for(xbuf.at[c], x_sem.at[c])

        @pl.when(s >= LATE)
        def _():
            wait_for(vin.at[c], v_sem.at[c])
            before = vin[c].astype(F32).reshape(T, KV).astype(BF16)
            for h in range(2):
                made = xbuf[c, h].astype(F32) + jnp.dot(before, wop[h], preferred_element_type=F32)
                xbuf[c, h] = made.astype(BF16)

        product = None
        squares = None
        scaled = []
        for h in range(2):
            floats = xbuf[c, h].astype(F32)
            scaled.append((floats * gain[h].astype(F32)).astype(BF16))
            sums = jnp.sum(floats * floats, axis=1, keepdims=True)
            squares = sums if h == 0 else squares + sums
            dot = jnp.dot(scaled[h], wv[h], preferred_element_type=F32)
            product = dot if h == 0 else product + dot
        both = with_pair(product, squares)
        part[c] = both.reshape(Y, OWN, EXT).astype(BF16)
        for offset in FAR_FIRST:
            rs_copy(c, offset).start()

        @pl.when((s >= LATE) & (s < 7) & jnp.logical_not(odd))
        def _():
            remote(xbuf.at[c, 1], xbuf.at[c, 1], send_sem.at[15], x_sem.at[c], (s + 1, d)).start()

        sc[rows_of(c), :] = jnp.where(core == 0, scaled[0], scaled[1])
        sct[c] = jnp.where(core == 0, scaled[1], scaled[0])
        remote(sct.at[c], sc.at[rows_of(c)], send_sem.at[6], give_sem.at[0], cpeer).start()

    def stage2(c):
        wait_for(rs.at[c], rs_sem.at[c])
        total = part[c, y].astype(F32)
        for j in range(Y - 1):
            total += rs[c, j].astype(F32)
        zs[c] = with_pair(total[:, :KV], pair_of(total)).astype(BF16)
        remote(zs.at[c], zr.at[c], send_sem.at[7], z_sem.at[c], zpeer).start()

    def stage3(c):
        wait_for(zr.at[c], z_sem.at[c])
        total = zs[c].astype(F32) + zr[c].astype(F32)
        inv = lax.rsqrt(pair_of(total) / D + 0.25)
        val[c, y] = with_pair(inv * total[:, :KV], inv).astype(BF16)

        @pl.when((s >= LATE - 1) & (s < 7))
        def _():
            for offset in (*FAR_FIRST, 0):
                remote(
                    val.at[c, y, :, pl.ds(0, KV)], vin.at[c, y], send_sem.at[13], v_sem.at[c], (s + 1, y_peer(offset)[1])
                ).start()

        for offset in FAR_FIRST:
            ag_copy(c, offset).start()

    def stage4(c):
        wait_for(rs.at[c], ag_sem.at[c])
        both = val[c].astype(F32).reshape(T, EXT)
        values = both[:, :KV].astype(BF16)
        for h in range(2):
            result = xbuf[c, h].astype(F32) + jnp.dot(values, wo[h], preferred_element_type=F32)
            outbuf[c, h] = result.astype(BF16)

        @pl.when(s < LATE - 1)
        def _():
            remote(outbuf.at[c], xbuf.at[c], send_sem.at[8], x_sem.at[c], (s + 1, d)).start()

        @pl.when((s >= LATE - 2) & (s < 6) & jnp.logical_not(odd))
        def _():
            remote(outbuf.at[c], xbuf.at[c], send_sem.at[14], x_sem.at[c], (s + 2, d)).start()

        @pl.when((s >= LATE - 2) & (s < 6) & odd)
        def _():
            remote(outbuf.at[c, 0], xbuf.at[c, 0], send_sem.at[14], x_sem.at[c], (s + 2, d)).start()

        wgt[rows_of(c), :] = (pair_of(both) * cot[c].astype(F32)).astype(BF16)
        remote(wgt.at[rows_of(c)], wgt.at[rows_of(c)], send_sem.at[9], give_sem.at[1], cpeer).start()
        pltpu.make_async_copy(outbuf.at[c, core], out_hbm.at[core, c], out_sem.at[0]).start()
        remote(outbuf.at[c, 1 - core], out_hbm.at[core, c], send_sem.at[10], out_sem.at[1], cpeer).start()

    def tick(k, carry):
        @pl.when(k == LAG4)
        def _():
            wait_for(wo, load_sem.at[1])
            load_cot.wait()

        def run(stage, lag, where=None):
            now = (k >= lag) & (k < NC + lag)

            @pl.when(now if where is None else now & where)
            def _():
                stage(k - lag)

        for stage, lag in ((stage1, 0),):
            run(stage, lag)
        run(stage4, LAGP, s >= LATE - 1)
        run(stage2, LAG2)
        run(stage3, LAG3)
        run(stage4, LAG4, s < LATE - 1)
        return carry

    lax.fori_loop(0, NC + LAGP, tick, 0)

    over_rows = (((0,), (0,)), ((), ()))
    over_cols = (((1,), (1,)), ((), ()))
    STEP = 256

    def block(i):
        return pl.ds(pl.multiple_of(i * STEP, STEP), STEP)

    other = pl.ds(pl.multiple_of((1 - core) * (ROWS // 2), ROWS // 2), ROWS // 2)
    wait_for(sc.at[other], give_sem.at[0])
    wait_for(wgt.at[other], give_sem.at[1])

    def grad_block(i, carry):
        gb[block(i), :] = lax.dot_general(
            sc[:, block(i)], wgt[...], over_rows, preferred_element_type=F32
        ).astype(BF16)
        return carry

    lax.fori_loop(0, W // STEP, grad_block, 0)

    half = KV // 2

    def right_rows(i, h):
        return lax.dot_general(
            gb[:, block(i)], gb[:, h * half : (h + 1) * half], over_rows, preferred_element_type=F32
        ).astype(BF16)

    def right_b(i, carry):
        rows = right_rows(i, 1)
        for j in range(4):
            rpb[j % 2, i // 2, 2 * lax.rem(i, 2) + j // 2] = rows[64 * j : 64 * (j + 1), :]
        return carry

    def right_a(i, carry):
        rows = right_rows(i, 0)
        for j in range(4):
            rpa[j % 2, 2 * lax.rem(i, 2) + j // 2, i // 2] = rows[64 * j : 64 * (j + 1), :]
        return carry

    core_b = remote(rpb.at[1 - core], r1b, rsend_sem.at[0], r_sem.at[0], cpeer)
    core_a = remote(rpa.at[1 - core], r1a, rsend_sem.at[1], r_sem.at[1], cpeer)
    lax.fori_loop(0, KV // STEP, right_b, 0)
    core_b.start()
    lax.fori_loop(0, KV // STEP, right_a, 0)
    core_a.start()

    def left_block(i, carry):
        add = lax.dot_general(gb[block(i), :], gb[...], over_cols, preferred_element_type=F32)
        left[block(i), :] = left[block(i), :] + add * (1.0 / 1024)
        return carry

    core_b.wait()
    r1b[...] = (rpb[core].astype(F32) + r1b[...].astype(F32)).astype(BF16)
    z_b = remote(r1b.at[1 - zl], r2b, rsend_sem.at[2], r_sem.at[2], zpeer)
    z_b.start()
    core_a.wait()
    r1a[...] = (rpa[core].astype(F32) + r1a[...].astype(F32)).astype(BF16)
    for offset in range(1, Y):
        remote(
            r1a.at[lax.rem(y + offset, Y)], r2a.at[offset - 1], rsend_sem.at[3], r_sem.at[3], y_peer(offset)
        ).start()
    load_left.wait()
    load_right.wait()
    lax.fori_loop(0, W // STEP, left_block, 0)
    left_copy = pltpu.make_async_copy(left, left_hbm, load_sem.at[3])
    left_copy.start()
    z_b.wait()
    tb[...] = (r1b[zl].astype(F32) + r2b[...].astype(F32)).astype(BF16)
    for offset in range(1, Y):
        remote(
            tb.at[lax.rem(y + offset, Y)], r3b.at[offset - 1], rsend_sem.at[4], r_sem.at[4], y_peer(offset)
        ).start()
    wait_for(r2a, r_sem.at[3])
    summed = r1a[y].astype(F32)
    for j in range(Y - 1):
        summed += r2a[j].astype(F32)
    ta[...] = summed.astype(BF16)
    z_a = remote(ta.at[1 - zl], r3a, rsend_sem.at[5], r_sem.at[5], zpeer)
    z_a.start()
    wait_for(r3b, r_sem.at[4])
    summed = tb[y].astype(F32)
    for j in range(Y - 1):
        summed += r3b[j].astype(F32)
    right[:, half:] = right[:, half:] + summed * (1.0 / D)
    z_a.wait()
    right[:, :half] = right[:, :half] + (ta[zl].astype(F32) + r3a[...].astype(F32)) * (1.0 / D)
    right_copy = pltpu.make_async_copy(right, right_hbm, load_sem.at[4])
    right_copy.start()

    wait_for(r2a, rsend_sem.at[3])
    wait_for(r3b, rsend_sem.at[4])
    wait_for(gain.at[0], send_sem.at[1])
    wait_for(wv.at[0], send_sem.at[2])
    wait_for(wo.at[0], send_sem.at[3])
    wait_for(rs, send_sem.at[4])
    wait_for(rs, send_sem.at[5])
    wait_for(sct, send_sem.at[6])
    wait_for(zs, send_sem.at[7])
    wait_for(wgt.at[other], send_sem.at[9])
    wait_for(sct, send_sem.at[10])
    wait_for(sct, out_sem.at[0])
    wait_for(sct, out_sem.at[1])

    @pl.when(s == 0)
    def _():
        wait_for(sct, send_sem.at[0])

    @pl.when(s < LATE - 1)
    def _():
        wait_for(outbuf, send_sem.at[8])

    @pl.when((s >= LATE - 2) & (s < 6) & jnp.logical_not(odd))
    def _():
        wait_for(outbuf, send_sem.at[14])

    @pl.when((s >= LATE - 2) & (s < 6) & odd)
    def _():
        wait_for(sct, send_sem.at[14])

    @pl.when((s >= LATE - 1) & (s < 7))
    def _():
        wait_for(wo.at[0], send_sem.at[11])
        wait_for(vin, send_sem.at[13])

    @pl.when(s >= LATE)
    def _():
        wait_for(wop.at[0], send_sem.at[12])

    @pl.when((s >= LATE) & (s < 7) & jnp.logical_not(odd))
    def _():
        wait_for(sct, send_sem.at[15])

    left_copy.wait()
    right_copy.wait()


def on_device(inputs, cotangent, norm_gain, value_weight, output_weight, left_old, right_old):
    any_space = pl.BlockSpec(memory_space=pl.ANY)
    dma = pltpu.SemaphoreType.DMA
    out, left, right = pl.pallas_call(
        kernel,
        out_shape=(
            jax.ShapeDtypeStruct((2, NC, T, W), BF16),
            jax.ShapeDtypeStruct((W, W), F32),
            jax.ShapeDtypeStruct((64, KV), F32),
        ),
        in_specs=[any_space] * 7,
        out_specs=(any_space, any_space, any_space),
        scratch_shapes=[
            pltpu.VMEM((2, W, KV), BF16),
            pltpu.VMEM((2, KV, W), BF16),
            pltpu.VMEM((2, KV, W), BF16),
            pltpu.VMEM((2, 1, W), BF16),
            pltpu.VMEM((NC, T, KV), BF16),
            pltpu.VMEM((NC, 2, T, W), BF16),
            pltpu.VMEM((NC, Y, OWN, KV), BF16),
            pltpu.VMEM((ROWS, W), BF16),
            pltpu.VMEM((NC, T, W), BF16),
            pltpu.VMEM((NC, 2, T, W), BF16),
            pltpu.VMEM((NC, Y, OWN, EXT), BF16),
            pltpu.VMEM((NC, Y - 1, OWN, EXT), BF16),
            pltpu.VMEM((NC, OWN, EXT), BF16),
            pltpu.VMEM((NC, OWN, EXT), BF16),
            pltpu.VMEM((NC, Y, OWN, EXT), BF16),
            pltpu.VMEM((ROWS, KV), BF16),
            pltpu.VMEM((W, KV), BF16),
            pltpu.VMEM((W, W), F32),
            pltpu.VMEM((64, KV), F32),
            pltpu.VMEM((2, Y, 2, 64, KV // 2), BF16),
            pltpu.VMEM((2, 2, Y, 64, KV // 2), BF16),
            pltpu.VMEM((Y, 2, 64, KV // 2), BF16),
            pltpu.VMEM((2, Y, 64, KV // 2), BF16),
            pltpu.VMEM((Y - 1, 2, 64, KV // 2), BF16),
            pltpu.VMEM((Y, 64, KV // 2), BF16),
            pltpu.VMEM((2, 64, KV // 2), BF16),
            pltpu.VMEM((Y, 64, KV // 2), BF16),
            pltpu.VMEM((64, KV // 2), BF16),
            pltpu.VMEM((Y - 1, 64, KV // 2), BF16),
            dma((6,)),
            dma((NC,)),
            dma((NC,)),
            dma((NC,)),
            dma((NC,)),
            dma((2,)),
            dma((2,)),
            dma((NC,)),
            dma((PIECES + 1,)),
            dma((16,)),
            dma((6,)),
            dma((6,)),
        ],
        compiler_params=pltpu.CompilerParams(
            collective_id=0, has_side_effects=True, vmem_limit_bytes=60 * 1024 * 1024,
        ),
    )(
        inputs.reshape(2, NC, T, W),
        cotangent.reshape(2, NC, T, KV),
        norm_gain,
        value_weight[0],
        output_weight[0],
        left_old[0, 0],
        right_old[0],
    )
    return out.reshape(1, 8, 128, W), left[None, None], right[None]


def solution(mesh):
    placed = (
        P(None, None, "dp"),
        P("section", None, None, None),
        P("section", "dp"),
        P("section", "dp", None),
        P("section", None, "dp"),
        P("section", "dp", None, None),
        P("section", "dp", None),
    )
    return jax.shard_map(
        on_device,
        mesh=mesh,
        in_specs=placed,
        out_specs=(
            P("section", None, None, "dp"),
            P("section", "dp", None, None),
            P("section", "dp", None),
        ),
        check_vma=False,
    )
```

```python
import jax
import jax.numpy as jnp
from jax import lax
from jax.experimental import pallas as pl
from jax.experimental.pallas import tpu as pltpu
from jax.sharding import PartitionSpec as P

MESH = pl.DeviceIdType.MESH
F32 = jnp.float32
BF16 = jnp.bfloat16

D = 16384
W = 1024
KV = 1024
ROWS = 1024
T = 32
NC = ROWS // 2 // T
Y = 4
FAR_FIRST = (2, 1, 3)
OWN = T // Y
EXT = KV + 128
LAG2, LAG3, LAG4 = 1, 2, 3
LAGP = 5
LATE = 4
PIECES = 4


def with_pair(rows, scalar):
    high = scalar.astype(BF16).astype(F32)
    low = scalar - high
    lane = lax.broadcasted_iota(jnp.int32, (rows.shape[0], 128), 1)
    pair = jnp.where(lane < 64, high, low)
    return jnp.concatenate([rows, pair], axis=1)


def pair_of(ext):
    return ext[:, KV : KV + 1] + ext[:, KV + 64 : KV + 65]


def kernel(
    x_hbm, cot_hbm, gain_ref, wv_hbm, wo_hbm, left_old_hbm, right_old_hbm,
    out_hbm, left_hbm, right_hbm,
    wv, wo, wop, gain, cot, xbuf, vin, sc, sct, outbuf, part, rs, zs, zr, val, wgt, gb, left, right,
    rpa, rpb, r1a, r1b, r2a, r2b, ta, tb, r3a, r3b,
    load_sem, x_sem, rs_sem, z_sem, ag_sem, out_sem, give_sem, v_sem, pre_sem, send_sem, r_sem, rsend_sem,
):
    s = lax.axis_index("section")
    d = lax.axis_index("dp")
    zl = d // 8
    core = lax.rem(d, 2)
    y = lax.rem(d, 8) // 2
    odd = lax.rem(s, 2) == 1
    zpeer = (s, lax.rem(d + 8, 16))
    cpeer = (s, d + 1 - 2 * core)

    def y_peer(offset):
        return (s, zl * 8 + lax.rem(y + offset, Y) * 2 + core)

    def rows_of(c):
        return pl.ds(pl.multiple_of(core * (ROWS // 2) + c * T, T), T)

    def remote(src, dst, send, recv, device):
        return pltpu.make_async_remote_copy(
            src_ref=src, dst_ref=dst, send_sem=send, recv_sem=recv, device_id=device, device_id_type=MESH
        )

    def wait_for(ref, sem):
        pltpu.make_async_copy(ref, ref, sem).wait()

    @pl.when(s == 0)
    def _():
        def body(c, carry):
            pltpu.make_async_copy(x_hbm.at[core, c], xbuf.at[c, core], x_sem.at[c]).start()
            return carry

        lax.fori_loop(0, NC, body, 0)

    pltpu.make_async_copy(wv_hbm, wv.at[core], load_sem.at[0]).start()
    pltpu.make_async_copy(wo_hbm, wo.at[core], load_sem.at[1]).start()
    load_cot = pltpu.make_async_copy(cot_hbm.at[core], cot, load_sem.at[2])
    load_left = pltpu.make_async_copy(left_old_hbm, left, load_sem.at[3])
    load_right = pltpu.make_async_copy(right_old_hbm, right, load_sem.at[4])
    pltpu.make_async_copy(gain_ref, gain.at[core], load_sem.at[5]).start()
    load_cot.start()
    load_left.start()
    load_right.start()

    barrier = pltpu.get_barrier_semaphore()
    for offset in range(1, Y):
        pl.semaphore_signal(barrier, inc=1, device_id=y_peer(offset), device_id_type=MESH)
    for step in (1, 7):
        for offset in range(Y):
            peer = (lax.rem(s + step, 8), y_peer(offset)[1])
            pl.semaphore_signal(barrier, inc=1, device_id=peer, device_id_type=MESH)
    for peer in (zpeer, cpeer, (lax.rem(s + 2, 8), d), (lax.rem(s + 6, 8), d)):
        pl.semaphore_signal(barrier, inc=1, device_id=peer, device_id_type=MESH)
    pl.semaphore_wait(barrier, Y - 1 + 2 * Y + 4)

    @pl.when(s == 0)
    def _():
        remote(x_hbm.at[1 - core, 0], xbuf.at[0, core], send_sem.at[0], x_sem.at[0], cpeer).start()

    remote(gain_ref, gain.at[core], send_sem.at[1], load_sem.at[5], cpeer).start()
    remote(wv_hbm, wv.at[core], send_sem.at[2], load_sem.at[0], cpeer).start()

    @pl.when(s == 0)
    def _():
        def body(c, carry):
            remote(x_hbm.at[1 - core, c], xbuf.at[c, core], send_sem.at[0], x_sem.at[c], cpeer).start()
            return carry

        lax.fori_loop(1, NC, body, 0)

    remote(wo_hbm, wo.at[core], send_sem.at[3], load_sem.at[1], cpeer).start()

    def piece(i):
        return pl.ds(i * (KV // PIECES), KV // PIECES)

    @pl.when((s >= LATE - 1) & (s < 7))
    def _():
        for i in range(PIECES):
            remote(
                wo_hbm.at[piece(i)], wop.at[core, piece(i)], send_sem.at[11], pre_sem.at[i], (s + 1, d)
            ).start()

    @pl.when(s >= LATE)
    def _():
        for i in range(PIECES):
            ours = wop.at[core, piece(i)]
            wait_for(ours, pre_sem.at[i])
            remote(ours, ours, send_sem.at[12], pre_sem.at[PIECES], cpeer).start()
        wait_for(wop.at[0], pre_sem.at[PIECES])

    wait_for(gain, load_sem.at[5])
    wait_for(wv, load_sem.at[0])

    def rs_copy(c, offset):
        return remote(
            part.at[c, lax.rem(y + offset, Y)], rs.at[c, offset - 1], send_sem.at[4], rs_sem.at[c], y_peer(offset)
        )

    def ag_copy(c, offset):
        return remote(val.at[c, y], val.at[c, y], send_sem.at[5], ag_sem.at[c], y_peer(offset))

    def stage1(c):
        wait_for(xbuf.at[c], x_sem.at[c])

        @pl.when(s >= LATE)
        def _():
            wait_for(vin.at[c], v_sem.at[c])
            before = vin[c].astype(F32).reshape(T, KV).astype(BF16)
            for h in range(2):
                made = xbuf[c, h].astype(F32) + jnp.dot(before, wop[h], preferred_element_type=F32)
                xbuf[c, h] = made.astype(BF16)

        product = None
        squares = None
        scaled = []
        for h in range(2):
            floats = xbuf[c, h].astype(F32)
            scaled.append((floats * gain[h].astype(F32)).astype(BF16))
            sums = jnp.sum(floats * floats, axis=1, keepdims=True)
            squares = sums if h == 0 else squares + sums
            dot = jnp.dot(scaled[h], wv[h], preferred_element_type=F32)
            product = dot if h == 0 else product + dot
        both = with_pair(product, squares)
        part[c] = both.reshape(Y, OWN, EXT).astype(BF16)
        for offset in FAR_FIRST:
            rs_copy(c, offset).start()

        @pl.when((s >= LATE) & (s < 7) & jnp.logical_not(odd))
        def _():
            remote(xbuf.at[c, 1], xbuf.at[c, 1], send_sem.at[15], x_sem.at[c], (s + 1, d)).start()

        sc[rows_of(c), :] = jnp.where(core == 0, scaled[0], scaled[1])
        sct[c] = jnp.where(core == 0, scaled[1], scaled[0])
        remote(sct.at[c], sc.at[rows_of(c)], send_sem.at[6], give_sem.at[0], cpeer).start()

    def stage2(c):
        wait_for(rs.at[c], rs_sem.at[c])
        total = part[c, y].astype(F32)
        for j in range(Y - 1):
            total += rs[c, j].astype(F32)
        zs[c] = with_pair(total[:, :KV], pair_of(total)).astype(BF16)
        remote(zs.at[c], zr.at[c], send_sem.at[7], z_sem.at[c], zpeer).start()

    def stage3(c):
        wait_for(zr.at[c], z_sem.at[c])
        total = zs[c].astype(F32) + zr[c].astype(F32)
        inv = lax.rsqrt(pair_of(total) / D + 0.25)
        val[c, y] = with_pair(inv * total[:, :KV], inv).astype(BF16)

        @pl.when((s >= LATE - 1) & (s < 7))
        def _():
            for offset in (*FAR_FIRST, 0):
                remote(
                    val.at[c, y, :, pl.ds(0, KV)], vin.at[c, y], send_sem.at[13], v_sem.at[c], (s + 1, y_peer(offset)[1])
                ).start()

        for offset in FAR_FIRST:
            ag_copy(c, offset).start()

    def stage4(c):
        wait_for(rs.at[c], ag_sem.at[c])
        both = val[c].astype(F32).reshape(T, EXT)
        values = both[:, :KV].astype(BF16)
        for h in range(2):
            result = xbuf[c, h].astype(F32) + jnp.dot(values, wo[h], preferred_element_type=F32)
            outbuf[c, h] = result.astype(BF16)

        @pl.when(s < LATE - 1)
        def _():
            remote(outbuf.at[c], xbuf.at[c], send_sem.at[8], x_sem.at[c], (s + 1, d)).start()

        @pl.when((s >= LATE - 2) & (s < 6) & jnp.logical_not(odd))
        def _():
            remote(outbuf.at[c], xbuf.at[c], send_sem.at[14], x_sem.at[c], (s + 2, d)).start()

        @pl.when((s >= LATE - 2) & (s < 6) & odd)
        def _():
            remote(outbuf.at[c, 0], xbuf.at[c, 0], send_sem.at[14], x_sem.at[c], (s + 2, d)).start()

        wgt[rows_of(c), :] = (pair_of(both) * cot[c].astype(F32)).astype(BF16)
        remote(wgt.at[rows_of(c)], wgt.at[rows_of(c)], send_sem.at[9], give_sem.at[1], cpeer).start()
        pltpu.make_async_copy(outbuf.at[c, core], out_hbm.at[core, c], out_sem.at[0]).start()
        remote(outbuf.at[c, 1 - core], out_hbm.at[core, c], send_sem.at[10], out_sem.at[1], cpeer).start()

    def tick(k, carry):
        @pl.when(k == LAG4)
        def _():
            wait_for(wo, load_sem.at[1])
            load_cot.wait()

        def run(stage, lag, where=None):
            now = (k >= lag) & (k < NC + lag)

            @pl.when(now if where is None else now & where)
            def _():
                stage(k - lag)

        for stage, lag in ((stage1, 0),):
            run(stage, lag)
        run(stage4, LAGP, s >= LATE - 1)
        run(stage2, LAG2)
        run(stage3, LAG3)
        run(stage4, LAG4, s < LATE - 1)
        return carry

    lax.fori_loop(0, NC + LAGP, tick, 0)

    over_rows = (((0,), (0,)), ((), ()))
    over_cols = (((1,), (1,)), ((), ()))
    STEP = 256

    def block(i):
        return pl.ds(pl.multiple_of(i * STEP, STEP), STEP)

    other = pl.ds(pl.multiple_of((1 - core) * (ROWS // 2), ROWS // 2), ROWS // 2)
    wait_for(sc.at[other], give_sem.at[0])
    wait_for(wgt.at[other], give_sem.at[1])

    def grad_block(i, carry):
        gb[block(i), :] = lax.dot_general(
            sc[:, block(i)], wgt[...], over_rows, preferred_element_type=F32
        ).astype(BF16)
        return carry

    lax.fori_loop(0, W // STEP, grad_block, 0)

    half = KV // 2

    def right_rows(i, h):
        return lax.dot_general(
            gb[:, block(i)], gb[:, h * half : (h + 1) * half], over_rows, preferred_element_type=F32
        ).astype(BF16)

    def right_b(i, carry):
        rows = right_rows(i, 1)
        for j in range(4):
            rpb[j % 2, i // 2, 2 * lax.rem(i, 2) + j // 2] = rows[64 * j : 64 * (j + 1), :]
        return carry

    def right_a(i, carry):
        rows = right_rows(i, 0)
        for j in range(4):
            rpa[j % 2, 2 * lax.rem(i, 2) + j // 2, i // 2] = rows[64 * j : 64 * (j + 1), :]
        return carry

    core_b = remote(rpb.at[1 - core], r1b, rsend_sem.at[0], r_sem.at[0], cpeer)
    core_a = remote(rpa.at[1 - core], r1a, rsend_sem.at[1], r_sem.at[1], cpeer)
    lax.fori_loop(0, KV // STEP, right_b, 0)
    core_b.start()
    lax.fori_loop(0, KV // STEP, right_a, 0)
    core_a.start()

    def left_block(i, carry):
        add = lax.dot_general(gb[block(i), :], gb[...], over_cols, preferred_element_type=F32)
        left[block(i), :] = left[block(i), :] + add * (1.0 / 1024)
        return carry

    core_b.wait()
    r1b[...] = (rpb[core].astype(F32) + r1b[...].astype(F32)).astype(BF16)
    z_b = remote(r1b.at[1 - zl], r2b, rsend_sem.at[2], r_sem.at[2], zpeer)
    z_b.start()
    core_a.wait()
    r1a[...] = (rpa[core].astype(F32) + r1a[...].astype(F32)).astype(BF16)
    for offset in FAR_FIRST:
        remote(
            r1a.at[lax.rem(y + offset, Y)], r2a.at[offset - 1], rsend_sem.at[3], r_sem.at[3], y_peer(offset)
        ).start()
    load_left.wait()
    load_right.wait()
    lax.fori_loop(0, W // STEP, left_block, 0)
    left_copy = pltpu.make_async_copy(left, left_hbm, load_sem.at[3])
    left_copy.start()
    z_b.wait()
    tb[...] = (r1b[zl].astype(F32) + r2b[...].astype(F32)).astype(BF16)
    for offset in FAR_FIRST:
        remote(
            tb.at[lax.rem(y + offset, Y)], r3b.at[offset - 1], rsend_sem.at[4], r_sem.at[4], y_peer(offset)
        ).start()
    wait_for(r2a, r_sem.at[3])
    summed = r1a[y].astype(F32)
    for j in range(Y - 1):
        summed += r2a[j].astype(F32)
    ta[...] = summed.astype(BF16)
    z_a = remote(ta.at[1 - zl], r3a, rsend_sem.at[5], r_sem.at[5], zpeer)
    z_a.start()
    wait_for(r3b, r_sem.at[4])
    summed = tb[y].astype(F32)
    for j in range(Y - 1):
        summed += r3b[j].astype(F32)
    right[:, half:] = right[:, half:] + summed * (1.0 / D)
    z_a.wait()
    right[:, :half] = right[:, :half] + (ta[zl].astype(F32) + r3a[...].astype(F32)) * (1.0 / D)
    right_copy = pltpu.make_async_copy(right, right_hbm, load_sem.at[4])
    right_copy.start()

    wait_for(r2a, rsend_sem.at[3])
    wait_for(r3b, rsend_sem.at[4])
    wait_for(gain.at[0], send_sem.at[1])
    wait_for(wv.at[0], send_sem.at[2])
    wait_for(wo.at[0], send_sem.at[3])
    wait_for(rs, send_sem.at[4])
    wait_for(rs, send_sem.at[5])
    wait_for(sct, send_sem.at[6])
    wait_for(zs, send_sem.at[7])
    wait_for(wgt.at[other], send_sem.at[9])
    wait_for(sct, send_sem.at[10])
    wait_for(sct, out_sem.at[0])
    wait_for(sct, out_sem.at[1])

    @pl.when(s == 0)
    def _():
        wait_for(sct, send_sem.at[0])

    @pl.when(s < LATE - 1)
    def _():
        wait_for(outbuf, send_sem.at[8])

    @pl.when((s >= LATE - 2) & (s < 6) & jnp.logical_not(odd))
    def _():
        wait_for(outbuf, send_sem.at[14])

    @pl.when((s >= LATE - 2) & (s < 6) & odd)
    def _():
        wait_for(sct, send_sem.at[14])

    @pl.when((s >= LATE - 1) & (s < 7))
    def _():
        wait_for(wo.at[0], send_sem.at[11])
        wait_for(vin, send_sem.at[13])

    @pl.when(s >= LATE)
    def _():
        wait_for(wop.at[0], send_sem.at[12])

    @pl.when((s >= LATE) & (s < 7) & jnp.logical_not(odd))
    def _():
        wait_for(sct, send_sem.at[15])

    left_copy.wait()
    right_copy.wait()


def on_device(inputs, cotangent, norm_gain, value_weight, output_weight, left_old, right_old):
    any_space = pl.BlockSpec(memory_space=pl.ANY)
    dma = pltpu.SemaphoreType.DMA
    out, left, right = pl.pallas_call(
        kernel,
        out_shape=(
            jax.ShapeDtypeStruct((2, NC, T, W), BF16),
            jax.ShapeDtypeStruct((W, W), F32),
            jax.ShapeDtypeStruct((64, KV), F32),
        ),
        in_specs=[any_space] * 7,
        out_specs=(any_space, any_space, any_space),
        scratch_shapes=[
            pltpu.VMEM((2, W, KV), BF16),
            pltpu.VMEM((2, KV, W), BF16),
            pltpu.VMEM((2, KV, W), BF16),
            pltpu.VMEM((2, 1, W), BF16),
            pltpu.VMEM((NC, T, KV), BF16),
            pltpu.VMEM((NC, 2, T, W), BF16),
            pltpu.VMEM((NC, Y, OWN, KV), BF16),
            pltpu.VMEM((ROWS, W), BF16),
            pltpu.VMEM((NC, T, W), BF16),
            pltpu.VMEM((NC, 2, T, W), BF16),
            pltpu.VMEM((NC, Y, OWN, EXT), BF16),
            pltpu.VMEM((NC, Y - 1, OWN, EXT), BF16),
            pltpu.VMEM((NC, OWN, EXT), BF16),
            pltpu.VMEM((NC, OWN, EXT), BF16),
            pltpu.VMEM((NC, Y, OWN, EXT), BF16),
            pltpu.VMEM((ROWS, KV), BF16),
            pltpu.VMEM((W, KV), BF16),
            pltpu.VMEM((W, W), F32),
            pltpu.VMEM((64, KV), F32),
            pltpu.VMEM((2, Y, 2, 64, KV // 2), BF16),
            pltpu.VMEM((2, 2, Y, 64, KV // 2), BF16),
            pltpu.VMEM((Y, 2, 64, KV // 2), BF16),
            pltpu.VMEM((2, Y, 64, KV // 2), BF16),
            pltpu.VMEM((Y - 1, 2, 64, KV // 2), BF16),
            pltpu.VMEM((Y, 64, KV // 2), BF16),
            pltpu.VMEM((2, 64, KV // 2), BF16),
            pltpu.VMEM((Y, 64, KV // 2), BF16),
            pltpu.VMEM((64, KV // 2), BF16),
            pltpu.VMEM((Y - 1, 64, KV // 2), BF16),
            dma((6,)),
            dma((NC,)),
            dma((NC,)),
            dma((NC,)),
            dma((NC,)),
            dma((2,)),
            dma((2,)),
            dma((NC,)),
            dma((PIECES + 1,)),
            dma((16,)),
            dma((6,)),
            dma((6,)),
        ],
        compiler_params=pltpu.CompilerParams(
            collective_id=0, has_side_effects=True, vmem_limit_bytes=60 * 1024 * 1024,
        ),
    )(
        inputs.reshape(2, NC, T, W),
        cotangent.reshape(2, NC, T, KV),
        norm_gain,
        value_weight[0],
        output_weight[0],
        left_old[0, 0],
        right_old[0],
    )
    return out.reshape(1, 8, 128, W), left[None, None], right[None]


def solution(mesh):
    placed = (
        P(None, None, "dp"),
        P("section", None, None, None),
        P("section", "dp"),
        P("section", "dp", None),
        P("section", None, "dp"),
        P("section", "dp", None, None),
        P("section", "dp", None),
    )
    return jax.shard_map(
        on_device,
        mesh=mesh,
        in_specs=placed,
        out_specs=(
            P("section", None, None, "dp"),
            P("section", "dp", None, None),
            P("section", "dp", None),
        ),
        check_vma=False,
    )
```
